256 devices in a mesh: dp: 32 (over x, z_lo, core), head: 8 (over y, z_hi).
Axes of the slice: x: 4, y: 4, z: 8 (z_hi: 2, z_lo: 4; z = z_hi * 4 + z_lo), core: 2. Of those that a mesh axis runs over, the one named last changes fastest.
Arguments:
- frames_in: bfloat16 [32, 8, 320, 640], P('dp', 'head'), may hold values from -6 to 6
- ln1_gain: float32 [1280], replicated, may hold values from 0.25 to 1.75
- ln1_bias: float32 [1280], replicated, may hold values from -3 to 3
- qkv_weight: bfloat16 [1280, 3, 1024], P('dp', None, 'head'), may hold values from -0.1875 to 0.1875
- qv_bias: float32 [2, 1024], P(None, 'head'), may hold values from -3 to 3
- out_weight: bfloat16 [1024, 1280], P(('head', 'dp')), may hold values from -0.1875 to 0.1875
- out_bias: float32 [1280], P('head'), may hold values from -3 to 3
- ln2_gain: float32 [1280], replicated, may hold values from 0.25 to 1.75
- ln2_bias: float32 [1280], replicated, may hold values from -3 to 3
- fc1_weight: bfloat16 [1280, 5120], P('dp', 'head'), may hold values from -0.15625 to 0.15625
- fc1_bias: float32 [5120], P('head'), may hold values from -3 to 3
- fc2_weight: bfloat16 [5120, 1280], P(('head', 'dp')), may hold values from -0.078125 to 0.078125
- fc2_bias: float32 [1280], P('head'), may hold values from -3 to 3
- server_of_clip: int32 [32], replicated, may hold values from 0 to 7
Outputs:
- encoded: bfloat16 [32, 8, 320, 640], P('dp', 'head')
The draws below stay inside these ranges and needn't reach their ends.
All inputs are finite; a program needn't handle non-finite values.
Results may differ from the reference program's by a relative error of at most 0.014.
Values may be sent and summed in bfloat16 or wider, within the bound.
A program may use at most 64 MiB of HBM per device.

```python
import jax
import jax.numpy as jnp
from jax import lax

D = 1280
HEADS = 16
HDIM = 64
MLP = 5120
FRAMES = 1280
SERVERS = 8
CLIPS = 32
N_HEAD = 8


def draw_qkv_weight(key, part):
    normal = jax.random.normal(jax.random.fold_in(key, 29), (D, 3, HEADS * HDIM), jnp.float32)
    return jnp.clip(normal * D ** (-0.5), -0.1875, 0.1875).astype(jnp.bfloat16)


def plant(entries, own_key, low, high):
    index_at = [jax.random.randint(jax.random.fold_in(own_key, axis), (), 0, length) for axis, length in enumerate(entries.shape)]
    widest = entries.shape.index(max(entries.shape))
    next_to = index_at[:widest] + [(index_at[widest] + 1) % entries.shape[widest]] + index_at[widest + 1:]
    return entries.at[tuple(index_at)].set(low).at[tuple(next_to)].set(high)


def block_levels(own_key, extent, split, low, top_value):
    level, own = 1.0, jax.random.fold_in(own_key, 6)
    for axis_at, shards_of in split:
        heights = jnp.exp(jax.random.uniform(jax.random.fold_in(own, axis_at), (shards_of,), jnp.float32, low / len(split), top_value / len(split)))
        level = level * jnp.repeat(heights, extent[axis_at] // shards_of).reshape([-1 if axis == axis_at else 1 for axis in range(len(extent))])
    return level


def noise(own_key, extent, deviation, most, split=(), held_as=jnp.bfloat16):
    level = block_levels(own_key, extent, split, -0.22, 0.18) if split else 1.0
    values = jax.random.normal(own_key, extent, jnp.float32) * deviation * level
    return jnp.minimum(jnp.maximum(values, -most), most).astype(held_as)


def setup_inputs(seed: int = 0) -> dict:
    streams_of = jax.random.split(jax.random.key(seed), 15)
    return {
        "frames_in": noise(streams_of[0], (CLIPS, N_HEAD, FRAMES // 4, 4 * D // N_HEAD), 1.0, 6.0, ((0, 32), (1, 8))),
        "ln1_gain": jnp.clip(1.0 + 0.15 * jax.random.normal(streams_of[1], (D,), jnp.float32), 0.25, 1.75),
        "ln1_bias": noise(streams_of[2], (D,), 0.5, 3.0, (), jnp.float32),
        "qkv_weight": draw_qkv_weight(jax.random.fold_in(streams_of[14], 71), 0),
        "qv_bias": noise(streams_of[4], (2, HEADS * HDIM), 0.5, 3.0, ((1, 8),), jnp.float32),
        "out_weight": noise(streams_of[5], (HEADS * HDIM, D), (HEADS * HDIM) ** -0.5, 0.1875, ((0, 256),)),
        "out_bias": noise(streams_of[6], (D,), 0.5, 3.0, ((0, 8),), jnp.float32),
        "ln2_gain": jnp.clip(1.0 + 0.15 * jax.random.normal(streams_of[7], (D,), jnp.float32), 0.25, 1.75),
        "ln2_bias": noise(streams_of[8], (D,), 0.5, 3.0, (), jnp.float32),
        "fc1_weight": noise(streams_of[9], (D, MLP), D ** -0.5, 0.15625, ((0, 32), (1, 8))),
        "fc1_bias": noise(streams_of[10], (MLP,), 0.5, 3.0, ((0, 8),), jnp.float32),
        "fc2_weight": noise(streams_of[11], (MLP, D), MLP ** -0.5, 0.078125, ((0, 256),)),
        "fc2_bias": noise(streams_of[12], (D,), 0.5, 3.0, ((0, 8),), jnp.float32),
        "server_of_clip": plant(jax.random.randint(streams_of[13], (CLIPS,), 0, SERVERS), jax.random.fold_in(streams_of[13], 1), 0, SERVERS - 1).astype(jnp.int32),
    }


epsilon = 1e-05

def layer_norm(matrix, gain_row, shift_row):
    floats = matrix.astype(jnp.float32)
    center = lax.optimization_barrier(jnp.mean(floats, axis=-1, keepdims=True))
    spread = lax.optimization_barrier(jnp.mean(jnp.square(floats - center), axis=-1, keepdims=True))
    return ((floats - center) * lax.rsqrt(spread + epsilon) * gain_row + shift_row).astype(jnp.bfloat16)

def attend(queries, key_rows, value_rows):

    def single(triple):
        query_head, key_head, value_head = triple
        scores = jnp.dot(query_head, key_head.T, preferred_element_type=jnp.float32)
        maxima = lax.optimization_barrier(jnp.max(scores, axis=-1, keepdims=True))
        weights = jnp.exp(scores - maxima)
        probability = (weights / lax.optimization_barrier(jnp.sum(weights, axis=-1, keepdims=True))).astype(jnp.bfloat16)
        return jnp.dot(probability, value_head, preferred_element_type=jnp.float32).astype(jnp.bfloat16)
    per_head = lax.map(single, (jnp.swapaxes(queries, 0, 1), jnp.swapaxes(key_rows, 0, 1), jnp.swapaxes(value_rows, 0, 1)))
    return jnp.swapaxes(per_head, 0, 1).reshape(queries.shape[0], -1)

def slot_order(server_list):
    clip_count = server_list.shape[0]
    indices = jnp.arange(clip_count, dtype=jnp.int32)
    earlier = (server_list[None, :] < server_list[:, None]) | (server_list[None, :] == server_list[:, None]) & (indices[None, :] < indices[:, None])
    slot_of = lax.optimization_barrier(jnp.sum(earlier.astype(jnp.int32), axis=1)).astype(jnp.int32)
    return lax.optimization_barrier(jnp.sum(jnp.where(slot_of[None, :] == indices[:, None], indices[None, :], 0), axis=1)).astype(jnp.int32)

def reference(frames_in, ln1_gain, ln1_bias, qkv_weight, qv_bias, out_weight, out_bias, ln2_gain, ln2_bias, fc1_weight, fc1_bias, fc2_weight, fc2_bias, server_of_clip):
    block_width = D // N_HEAD
    clip_total = frames_in.shape[0]
    residual_all = frames_in.reshape(clip_total, N_HEAD, FRAMES // 4, 4, block_width).transpose(0, 2, 3, 1, 4).reshape(clip_total, FRAMES, D)

    def clip_layer(residual_in):
        frame_count = residual_in.shape[0]
        normed_one = layer_norm(residual_in, ln1_gain, ln1_bias)
        column_count = qkv_weight.shape[2]
        projected = jnp.dot(normed_one, qkv_weight.reshape(qkv_weight.shape[0], 3 * column_count), preferred_element_type=jnp.float32).reshape(frame_count, 3, column_count)
        queries = ((projected[:, 0] + qv_bias[0]) * HDIM ** (-0.5)).astype(jnp.bfloat16).reshape(frame_count, -1, HDIM)
        key_rows = projected[:, 1].astype(jnp.bfloat16).reshape(frame_count, -1, HDIM)
        value_rows = (projected[:, 2] + qv_bias[1]).astype(jnp.bfloat16).reshape(frame_count, -1, HDIM)
        context = attend(queries, key_rows, value_rows)
        attended = (residual_in.astype(jnp.float32) + out_bias + jnp.dot(context, out_weight, preferred_element_type=jnp.float32)).astype(jnp.bfloat16)
        normed_two = layer_norm(attended, ln2_gain, ln2_bias)
        hidden = jax.nn.gelu(jnp.dot(normed_two, fc1_weight, preferred_element_type=jnp.float32) + fc1_bias, approximate=False).astype(jnp.bfloat16)
        return (attended.astype(jnp.float32) + fc2_bias + jnp.dot(hidden, fc2_weight, preferred_element_type=jnp.float32)).astype(jnp.bfloat16)
    layer_out = lax.map(clip_layer, residual_all)
    clip_order = slot_order(server_of_clip)
    ordered = jnp.take(layer_out, clip_order, axis=0)
    return ordered.reshape(clip_total, FRAMES // 4, 4, N_HEAD, block_width).transpose(0, 3, 1, 2, 4).reshape(clip_total, N_HEAD, FRAMES // 4, 4 * block_width)
```

```python
import functools

import jax
import jax.numpy as jnp
from jax import lax
from jax.experimental import pallas as pl
from jax.experimental.pallas import tpu as pltpu
from jax.sharding import Mesh
from jax.sharding import PartitionSpec as P

MESH = pl.DeviceIdType.MESH
BF16 = jnp.bfloat16
F32 = jnp.float32
EPS = 1e-05
HDIM = 64
DP = ("x", "zl", "c")
HEAD = ("y", "zh")
HEAD_DP = ("y", "zh", "x", "zl", "c")

D = 1280
HALF = 160
TILES = 112
PIECE = 7


def remote(src, dst, send, recv, device):
    return pltpu.make_async_remote_copy(
        src_ref=src, dst_ref=dst, send_sem=send, recv_sem=recv,
        device_id=device, device_id_type=MESH,
    )


class Ring4:
    def __init__(self, slab, half, i, device, send, recv, first=None):
        up, down = lax.rem(i + 1, 4), lax.rem(i + 3, 4)
        own = slab(i)
        self.one = [
            remote(own, own, send.at[0], recv.at[0], device(up)),
            remote(own, own, send.at[1], recv.at[1], device(down)),
        ]
        self.two = [
            remote(half(down, 0), half(down, 0), send.at[2], recv.at[2], device(up)),
            remote(half(up, 1), half(up, 1), send.at[3], recv.at[3], device(down)),
        ]

    def start(self):
        for copy in self.one:
            copy.start()

    def forward(self):
        for copy, nxt in zip(self.one, self.two):
            copy.wait_recv()
            nxt.start()

    def arrive(self):
        for copy in self.two:
            copy.wait_recv()

    def drain(self):
        for copy in self.one + self.two:
            copy.wait_send()


class Ring8:
    def __init__(self, slab, i, device, send, recv):
        up, down = lax.rem(i + 1, 8), lax.rem(i + 7, 8)
        self.steps = []
        for s in range(4):
            older = slab(lax.rem(i + 8 - s, 8))
            copies = [remote(older, older, send.at[2 * s], recv.at[2 * s], device(up))]
            if s < 3:
                newer = slab(lax.rem(i + s, 8))
                copies.append(
                    remote(newer, newer, send.at[2 * s + 1], recv.at[2 * s + 1], device(down))
                )
            self.steps.append(copies)

    def start(self, s):
        for copy in self.steps[s]:
            copy.start()

    def arrive(self, s):
        for copy in self.steps[s]:
            copy.wait_recv()

    def drain(self):
        for copies in self.steps:
            for copy in copies:
                copy.wait_send()


def layer_norm(floats, gain, shift):
    center = jnp.sum(floats, axis=-1, keepdims=True) * (1.0 / D)
    moved = floats - center
    spread = jnp.sum(moved * moved, axis=-1, keepdims=True) * (1.0 / D)
    return (moved * lax.rsqrt(spread + EPS) * gain + shift).astype(BF16)


def dot(a, b):
    return jnp.dot(a, b, preferred_element_type=F32)


def kernel(
    order, fin, qkv_in, fc1_in, tail_in, bias_in, norms,
    out,
    p1, p2, xg, wq, w1, w2, wo, pair, bg, xr, xn, qs, kv, cx, att, n2, pk, ra, rb, rc, rd, fo,
    local, s_p1, r_p1, s_p2, r_p2, s_pair, r_pair, s_bias, r_bias,
    s_zq, r_zq, s_zo, r_zo, s_z1, r_z1, s_z2, r_z2,
    s_xq, r_xq, s_xo, r_xo, s_x1, r_x1, s_x2, r_x2,
    s_yx, r_yx, s_yo, r_yo, s_yn, r_yn, s_d, r_d, s_cx, r_cx, s_rs, r_rs, s_out, r_out,
):
    x, zl, c = lax.axis_index("x"), lax.axis_index("zl"), lax.axis_index("c")
    y, zh = lax.axis_index("y"), lax.axis_index("zh")
    z = zh * 4 + zl
    clip = x * 8 + zl * 2 + c

    def at(x_=x, zl_=zl, c_=c, y_=y, zh_=zh):
        return (x_, zl_, c_, y_, zh_)

    def at_z(z_):
        return at(zl_=lax.rem(z_, 4), zh_=z_ // 4)

    sibling = at(c_=1 - c)

    barrier = pltpu.get_barrier_semaphore()

    def greet(device):
        pl.semaphore_signal(barrier, inc=1, device_id=device, device_id_type=MESH)

    @pl.loop(1, 32)
    def _(i):
        t = lax.rem(clip + i, 32)
        greet(at(x_=t // 8, zl_=lax.rem(t // 2, 4), c_=lax.rem(t, 2)))

    @pl.loop(0, 16)
    def _(i):
        t = lax.rem(x * 4 + zl + i, 16)
        greet(at(x_=t // 4, zl_=lax.rem(t, 4), zh_=1 - zh))

    greet(at(c_=1 - c, zh_=1 - zh))
    for i in range(1, 4):
        greet(at(y_=lax.rem(y + i, 4)))
        greet(at(y_=lax.rem(y + i, 4), zh_=1 - zh))
    pl.semaphore_wait(barrier, 54)

    to_pair = remote(tail_in.at[1 - c], pair.at[c], s_pair, r_pair, sibling)
    to_pair.start()
    own_pair = pltpu.make_async_copy(tail_in.at[c], pair.at[c], local.at[0])

    def piece_of(x_, zl_, c_):
        return c_ * 16 + x_ * 4 + zl_

    @pl.loop(1, 32)
    def _(i):
        t = lax.rem(clip + i, 32)
        x_, zl_, c_ = t // 8, lax.rem(t // 2, 4), lax.rem(t, 2)
        remote(fin.at[piece_of(x_, zl_, c_)], p1.at[clip], s_p1, r_p1, at(x_=x_, zl_=zl_, c_=c_)).start()

    keep_one = pltpu.make_async_copy(fin.at[piece_of(x, zl, c)], p1.at[clip], r_p1)
    keep_one.start()

    own_q = pltpu.make_async_copy(qkv_in, wq.at[zh, x, zl, c], local.at[1])
    own_1 = pltpu.make_async_copy(fc1_in, w1.at[zh, x, zl, c], local.at[2])
    own_b = pltpu.make_async_copy(bias_in, bg.at[y * 2 + zh], local.at[3])
    for copy in (own_q, own_1, own_b):
        copy.start()

    bias_sends = []
    for i in range(4):
        for other in range(2):
            if i or other:
                device = at(y_=lax.rem(y + i, 4), zh_=(1 - zh) if other else zh)
                n = i * 2 + other
                bias_sends.append(
                    remote(bias_in, bg.at[y * 2 + zh], s_bias.at[n], r_bias.at[n], device)
                )

    zq = Ring8(lambda i: wq.at[i // 4, x, lax.rem(i, 4), c], z, at_z, s_zq, r_zq)
    zo = Ring8(lambda i: wo.at[c, y, i // 4, x, lax.rem(i, 4)], z, at_z, s_zo, r_zo)
    z1 = Ring8(lambda i: w1.at[i // 4, x, lax.rem(i, 4), c], z, at_z, s_z1, r_z1)
    z2 = Ring8(lambda i: w2.at[c, i // 4, x, lax.rem(i, 4)], z, at_z, s_z2, r_z2)

    def at_x(i):
        return at(x_=i)

    def at_y(i):
        return at(y_=i)

    xq = Ring4(lambda i: wq.at[:, i, :, c], lambda i, h: wq.at[h, i, :, c], x, at_x, s_xq, r_xq)
    xo = Ring4(lambda i: wo.at[c, y, :, i], lambda i, h: wo.at[c, y, h, i], x, at_x, s_xo, r_xo)
    x1 = Ring4(lambda i: w1.at[:, i, :, c], lambda i, h: w1.at[h, i, :, c], x, at_x, s_x1, r_x1)
    x2 = Ring4(lambda i: w2.at[c, :, i], lambda i, h: w2.at[c, h, i], x, at_x, s_x2, r_x2)
    yx = Ring4(
        lambda i: xg.at[i, :, pl.ds(0, 100)],
        lambda i, h: xg.at[i, h, pl.ds(0, 100)],
        y, at_y, s_yx, r_yx,
    )
    yo = Ring4(lambda i: wo.at[c, i], lambda i, h: wo.at[c, i, h], y, at_y, s_yo, r_yo)
    yn = Ring4(
        lambda i: n2.at[i], lambda i, h: n2.at[i, pl.ds(80 * h, 80)], y, at_y, s_yn, r_yn
    )
    dq = remote(wq.at[:, :, :, c], wq.at[:, :, :, c], s_d.at[0], r_d.at[0], sibling)
    do = remote(wo.at[c], wo.at[c], s_d.at[1], r_d.at[1], sibling)
    d1 = remote(w1.at[:, :, :, c], w1.at[:, :, :, c], s_d.at[2], r_d.at[2], sibling)
    d2 = remote(w2.at[c], w2.at[c], s_d.at[3], r_d.at[3], sibling)
    dkv = remote(kv.at[c], kv.at[c], s_d.at[4], r_d.at[4], sibling)

    own_q.wait()
    zq.start(0)
    for copy in bias_sends:
        copy.start()
    own_pair.start()
    own_pair.wait()
    to_pair.wait_recv()
    wo[c, y, zh, x, zl, 0:4] = pair[0, 0:4]
    wo[c, y, zh, x, zl, 4:8] = pair[1, 0:4]
    w2[c, zh, x, zl, 0:20] = pair[0, 4:24]
    w2[c, zh, x, zl, 20:40] = pair[1, 4:24]
    zo.start(0)
    for s in range(4):
        zq.arrive(s)
        zo.arrive(s)
        if s < 3:
            zq.start(s + 1)
            zo.start(s + 1)
    own_1.wait()
    own_b.wait()

    pltpu.make_async_copy(p1, p1, r_p1).wait()

    @pl.loop(0, 32)
    def _(s):
        p2[s] = p1[order[s]]

    slot = x * 8 + zl * 2 + zh
    place = xg.at[y, zh, pl.ds(PIECE * (x * 4 + zl), PIECE)]

    @pl.loop(1, 32)
    def _(i):
        t = lax.rem(slot + i, 32)
        remote(
            p2.at[t], place, s_p2, r_p2, at(x_=t // 8, zl_=lax.rem(t // 2, 4), zh_=lax.rem(t, 2))
        ).start()

    keep_two = pltpu.make_async_copy(p2.at[slot], place, r_p2)
    keep_two.start()

    xq.start()
    xo.start()
    z1.start(0)
    z2.start(0)
    xq.forward()
    xo.forward()
    pltpu.make_async_copy(xg.at[y], xg.at[y], r_p2).wait()
    yx.start()
    for s in range(4):
        z1.arrive(s)
        z2.arrive(s)
        if s < 3:
            z1.start(s + 1)
            z2.start(s + 1)
        if s == 0:
            xq.arrive()
            dq.start()
        if s == 1:
            yx.forward()
    x1.start()
    x2.start()
    for copy in bias_sends:
        copy.wait_recv()
    yx.arrive()

    @pl.loop(0, 10)
    def _(t):
        rows = []
        for b in range(8):
            parts = [
                xg[b // 2, b % 2, pl.ds(lt * 20 + t * 2, 2)].reshape(16, 128) for lt in range(5)
            ]
            rows.append(jnp.concatenate(parts, axis=1))
        for j in range(4):
            whole = jnp.concatenate([r[:, 160 * j : 160 * j + 160] for r in rows], axis=1)
            start = pl.multiple_of(t * 16, 16)
            xr[j, pl.ds(start, 16)] = whole
            xn[j, pl.ds(start, 16)] = layer_norm(whole.astype(F32), norms[0:1], norms[1:2])

    dq.wait_recv()

    @pl.loop(0, 4)
    def _(j):
        left = xn[j]
        rows = pl.ds(pl.multiple_of(j * HALF, HALF), HALF)
        for h in range(2):
            prod = dot(left, wq[h].reshape(D, 384))
            biases = bg[y * 2 + h]
            lanes = slice(128 * h, 128 * h + 128)
            qs[rows, lanes] = ((prod[:, 0:128] + biases[3:4, 0:128]) * HDIM ** (-0.5)).astype(BF16)
            kv[c, 0, rows, lanes] = prod[:, 128:256].astype(BF16)
            kv[c, 1, rows, lanes] = (prod[:, 256:384] + biases[4:5, 0:128]).astype(BF16)

    dkv.start()
    xo.arrive()
    yo.start()
    dkv.wait_recv()

    head_of = lax.broadcasted_iota(jnp.int32, (HALF, 256), 1) // HDIM

    def attend(j):
        rows = pl.ds(pl.multiple_of(j * HALF, HALF), HALF)
        q = qs[rows, :]
        zero = jnp.zeros_like(q)
        stacked = jnp.concatenate([jnp.where(head_of == h, q, zero) for h in range(4)], axis=0)
        keys = kv[:, 0].reshape(D, 256)
        scores = lax.dot_general(
            stacked, keys, (((1,), (1,)), ((), ())), preferred_element_type=F32
        )
        weights = jnp.exp(scores - jnp.max(scores, axis=-1, keepdims=True))
        total = jnp.sum(weights, axis=-1, keepdims=True)
        mixed = dot(weights.astype(BF16), kv[:, 1].reshape(D, 256)) / total
        context = jnp.zeros((HALF, 256), F32)
        for h in range(4):
            context = context + jnp.where(head_of == h, mixed[h * HALF : (h + 1) * HALF], 0.0)
        return context.astype(BF16)

    @pl.loop(1, 4)
    def _(i):
        j = lax.rem(y + i, 4)
        cx[4 + j] = attend(j)
        remote(cx.at[4 + j], cx.at[y], s_cx.at[i - 1], r_cx.at[i - 1], at(y_=j)).start()

    yo.forward()
    cx[y] = attend(y)
    x1.forward()
    x2.forward()
    yo.arrive()
    do.start()
    for i in range(1, 4):
        remote(cx.at[0], cx.at[0], s_cx.at[i - 1], r_cx.at[i - 1], sibling).wait_recv()
    do.wait_recv()

    def whole_bias(row):
        return jnp.concatenate([bg[h, row : row + 1, 0:160] for h in range(8)], axis=1)

    context = jnp.concatenate([cx[i] for i in range(4)], axis=1)
    product = jnp.concatenate(
        [dot(context, wo[h].reshape(1024, 640)) for h in range(2)], axis=1
    )
    attended = (xr[y].astype(F32) + whole_bias(1) + product).astype(BF16)
    att[...] = attended.astype(F32) + whole_bias(2)
    n2[y] = layer_norm(attended.astype(F32), norms[2:3], norms[3:4])
    yn.start()
    x1.arrive()
    x2.arrive()
    d1.start()
    d2.start()
    yn.forward()
    d1.wait_recv()
    d2.wait_recv()
    yn.arrive()

    for j in range(4):
        left = n2[j]
        parts = []
        for h in range(2):
            sums = dot(left, w1[h].reshape(D, 640)) + bg[y * 2 + h, 0:1, :]
            parts.append((0.5 * sums * (1.0 + lax.erf(sums * 0.5**0.5))).astype(BF16))
        hidden = jnp.concatenate(parts, axis=1)
        share = jnp.concatenate(
            [dot(hidden, w2[h].reshape(D, 640)) for h in range(2)], axis=1
        )
        share = share + jnp.where(y == j, att[...], 0.0)
        for b in range(8):
            pk[b // 2, b % 2, :, 160 * j : 160 * j + 160] = share[:, 160 * b : 160 * b + 160].astype(
                BF16
            )

    up, down, far = lax.rem(y + 1, 4), lax.rem(y + 3, 4), lax.rem(y + 2, 4)
    sums = [
        remote(pk.at[far, 0], ra, s_rs.at[0], r_rs.at[0], at(y_=up)),
        remote(pk.at[far, 1], rb, s_rs.at[1], r_rs.at[1], at(y_=down)),
        remote(pk.at[up], rc, s_rs.at[2], r_rs.at[2], at(y_=up)),
        remote(pk.at[down], rd, s_rs.at[3], r_rs.at[3], at(y_=down)),
    ]
    sums[0].start()
    sums[1].start()
    sums[0].wait_recv()
    pk[up, 0] = (pk[up, 0].astype(F32) + ra[...].astype(F32)).astype(BF16)
    sums[2].start()
    sums[1].wait_recv()
    pk[down, 1] = (pk[down, 1].astype(F32) + rb[...].astype(F32)).astype(BF16)
    sums[3].start()
    sums[2].wait_recv()
    sums[3].wait_recv()
    fo[...] = (pk[y].astype(F32) + rc[...].astype(F32) + rd[...].astype(F32)).astype(BF16)

    mine = pl.ds(pl.multiple_of(c * HALF, HALF), HALF)
    across = remote(fo.at[1 - zh], out.at[mine], s_out.at[0], r_out, at(c_=zh, zh_=1 - zh))
    across.start()
    keep_out = pltpu.make_async_copy(fo.at[zh], out.at[mine], r_out)
    beside = remote(fo.at[zh], out.at[mine], s_out.at[1], r_out, sibling)

    @pl.when(c == zh)
    def _():
        keep_out.start()

    @pl.when(c != zh)
    def _():
        beside.start()

    pltpu.make_async_copy(out, out, r_out).wait()

    across.wait_send()

    @pl.when(c != zh)
    def _():
        beside.wait_send()

    to_pair.wait_send()
    pltpu.make_async_copy(p1.at[pl.ds(0, 31)], p1.at[pl.ds(0, 31)], s_p1).wait()
    pltpu.make_async_copy(p1.at[pl.ds(0, 31)], p1.at[pl.ds(0, 31)], s_p2).wait()
    for copy in bias_sends + sums + [dq, do, d1, d2, dkv]:
        copy.wait_send()
    for i in range(1, 4):
        remote(cx.at[0], cx.at[0], s_cx.at[i - 1], r_cx.at[i - 1], sibling).wait_send()
    for ring in (zq, zo, z1, z2, xq, xo, x1, x2, yx, yo, yn):
        ring.drain()


def slot_order(server_list):
    clip_count = server_list.shape[0]
    indices = jnp.arange(clip_count, dtype=jnp.int32)
    earlier = (server_list[None, :] < server_list[:, None]) | (
        server_list[None, :] == server_list[:, None]
    ) & (indices[None, :] < indices[:, None])
    slot_of = jnp.sum(earlier.astype(jnp.int32), axis=1)
    return jnp.sum(jnp.where(slot_of[None, :] == indices[:, None], indices[None, :], 0), axis=1)


def on_device(
    frames_in, ln1_gain, ln1_bias, qkv_weight, qv_bias, out_weight, out_bias,
    ln2_gain, ln2_bias, fc1_weight, fc1_bias, fc2_weight, fc2_bias, server_of_clip,
):
    clip_order = slot_order(server_of_clip)
    tiles = frames_in[0, 0].reshape(2, 20, 8, 5, 128).transpose(0, 3, 1, 2, 4)
    fin = jnp.pad(tiles.reshape(2, 100, 8, 128), ((0, 0), (0, TILES - 100), (0, 0), (0, 0)))
    fin = fin.reshape(32, PIECE, 8, 128)
    tail = jnp.concatenate([out_weight, fc2_weight], axis=0).reshape(24, 2, 640).transpose(1, 0, 2)

    def row(v):
        return jnp.pad(v, (0, 640 - v.shape[0]))[None]

    biases = jnp.concatenate(
        [row(fc1_bias), row(out_bias), row(fc2_bias), row(qv_bias[0]), row(qv_bias[1]),
         jnp.zeros((3, 640), F32)], axis=0,
    )
    norms = jnp.stack([ln1_gain, ln1_bias, ln2_gain, ln2_bias])
    vmem = pl.BlockSpec(memory_space=pltpu.VMEM)
    smem = pl.BlockSpec(memory_space=pltpu.SMEM)
    dma = pltpu.SemaphoreType.DMA
    V = pltpu.VMEM
    out = pl.pallas_call(
        kernel,
        out_shape=jax.ShapeDtypeStruct((320, 640), BF16),
        in_specs=[smem] + [vmem] * 6,
        out_specs=vmem,
        scratch_shapes=[
            V((32, PIECE, 8, 128), BF16),
            V((32, PIECE, 8, 128), BF16),
            V((4, 2, TILES, 8, 128), BF16),
            V((2, 4, 4, 2, 40, 384), BF16),
            V((2, 4, 4, 2, 40, 640), BF16),
            V((2, 2, 4, 4, 40, 640), BF16),
            V((2, 4, 2, 4, 4, 8, 640), BF16),
            V((2, 24, 640), BF16),
            V((8, 8, 640), F32),
            V((4, HALF, D), BF16),
            V((4, HALF, D), BF16),
            V((640, 256), BF16),
            V((2, 2, 640, 256), BF16),
            V((8, HALF, 256), BF16),
            V((HALF, D), F32),
            V((4, HALF, D), BF16),
            V((4, 2, HALF, 640), BF16),
            V((HALF, 640), BF16),
            V((HALF, 640), BF16),
            V((2, HALF, 640), BF16),
            V((2, HALF, 640), BF16),
            V((2, HALF, 640), BF16),
            dma((4,)),
            dma, dma, dma, dma, dma, dma, dma((8,)), dma((8,)),
            dma((7,)), dma((7,)), dma((7,)), dma((7,)), dma((7,)), dma((7,)), dma((7,)), dma((7,)),
            dma((4,)), dma((4,)), dma((4,)), dma((4,)), dma((4,)), dma((4,)), dma((4,)), dma((4,)),
            dma((4,)), dma((4,)), dma((4,)), dma((4,)), dma((4,)), dma((4,)),
            dma((5,)), dma((5,)), dma((3,)), dma((3,)), dma((4,)), dma((4,)), dma((2,)), dma,
        ],
        compiler_params=pltpu.CompilerParams(
            collective_id=0, has_side_effects=True, vmem_limit_bytes=60 * 2**20
        ),
    )(clip_order, fin, qkv_weight.reshape(40, 384), fc1_weight, tail, biases, norms)
    return out.reshape(1, 1, 320, 640)


def solution(mesh):
    torus = Mesh(mesh.devices.reshape(4, 4, 2, 4, 2), ("x", "zl", "c", "y", "zh"))
    return jax.shard_map(
        on_device,
        mesh=torus,
        in_specs=(
            P(DP, HEAD, None, None), P(), P(), P(DP, None, HEAD), P(None, HEAD), P(HEAD_DP, None),
            P(HEAD), P(), P(), P(DP, HEAD), P(HEAD), P(HEAD_DP, None), P(HEAD), P(),
        ),
        out_specs=P(DP, HEAD, None, None),
        check_vma=False,
    )
```

```python
import functools

import jax
import jax.numpy as jnp
from jax import lax
from jax.experimental import pallas as pl
from jax.experimental.pallas import tpu as pltpu
from jax.sharding import Mesh
from jax.sharding import PartitionSpec as P

MESH = pl.DeviceIdType.MESH
BF16 = jnp.bfloat16
F32 = jnp.float32
EPS = 1e-05
HDIM = 64
DP = ("x", "zl", "c")
HEAD = ("y", "zh")
HEAD_DP = ("y", "zh", "x", "zl", "c")

D = 1280
HALF = 160
TILES = 112
PIECE = 7
CHUNKS = 5
ROWS = 32


def remote(src, dst, send, recv, device):
    return pltpu.make_async_remote_copy(
        src_ref=src, dst_ref=dst, send_sem=send, recv_sem=recv,
        device_id=device, device_id_type=MESH,
    )


class Ring4:
    def __init__(self, slab, half, i, device, send, recv, base=0):
        up, down = lax.rem(i + 1, 4), lax.rem(i + 3, 4)
        own = slab(i)

        def sems(n):
            return send.at[base + n], recv.at[base + n]

        self.one = [
            remote(own, own, *sems(0), device(up)),
            remote(own, own, *sems(1), device(down)),
        ]
        self.two = [
            remote(half(down, 0), half(down, 0), *sems(2), device(up)),
            remote(half(up, 1), half(up, 1), *sems(3), device(down)),
        ]

    def start(self):
        for copy in self.one:
            copy.start()

    def forward(self):
        for copy, nxt in zip(self.one, self.two):
            copy.wait_recv()
            nxt.start()

    def arrive(self):
        for copy in self.two:
            copy.wait_recv()

    def drain(self):
        for copy in self.one + self.two:
            copy.wait_send()


class Ring8:
    def __init__(self, slab, i, device, send, recv):
        up, down = lax.rem(i + 1, 8), lax.rem(i + 7, 8)
        self.steps = []
        for s in range(4):
            older = slab(lax.rem(i + 8 - s, 8))
            copies = [remote(older, older, send.at[2 * s], recv.at[2 * s], device(up))]
            if s < 3:
                newer = slab(lax.rem(i + s, 8))
                copies.append(
                    remote(newer, newer, send.at[2 * s + 1], recv.at[2 * s + 1], device(down))
                )
            self.steps.append(copies)

    def start(self, s):
        for copy in self.steps[s]:
            copy.start()

    def arrive(self, s):
        for copy in self.steps[s]:
            copy.wait_recv()

    def relay(self, s):
        self.arrive(s)
        if s < 3:
            self.start(s + 1)

    def drain(self):
        for copies in self.steps:
            for copy in copies:
                copy.wait_send()


def layer_norm(floats, gain, shift):
    center = jnp.sum(floats, axis=-1, keepdims=True) * (1.0 / D)
    moved = floats - center
    spread = jnp.sum(moved * moved, axis=-1, keepdims=True) * (1.0 / D)
    return (moved * lax.rsqrt(spread + EPS) * gain + shift).astype(BF16)


def dot(a, b):
    return jnp.dot(a, b, preferred_element_type=F32)


def kernel(
    order, frames, qkv_in, fc1_in, out_in, fc2_in, b_qv, b_out, b_fc1, b_fc2, g1, s1, g2, s2,
    out,
    fin, p1, p2, xg, wq, w1, w2, wo, tail, pair, bias, bg, xr, xn, qs, kv, cx, att, n2, pk,
    ra, rb, rc, rd, fo,
    local, s_p1, r_p1, s_p2, r_p2, s_pair, r_pair, s_bias, r_bias,
    s_zq, r_zq, s_zo, r_zo, s_z1, r_z1, s_z2, r_z2,
    s_xq, r_xq, s_xo, r_xo, s_x1, r_x1, s_x2, r_x2,
    s_yx, r_yx, s_yo, r_yo, s_yn, r_yn, s_d, r_d, s_cx, r_cx, s_rs, r_rs, s_out, s_next, r_out,
):
    x, zl, c = lax.axis_index("x"), lax.axis_index("zl"), lax.axis_index("c")
    y, zh = lax.axis_index("y"), lax.axis_index("zh")
    z = zh * 4 + zl
    clip = x * 8 + zl * 2 + c

    def at(x_=x, zl_=zl, c_=c, y_=y, zh_=zh):
        return (x_, zl_, c_, y_, zh_)

    def at_z(z_):
        return at(zl_=lax.rem(z_, 4), zh_=z_ // 4)

    def at_x(i):
        return at(x_=i)

    def at_y(i):
        return at(y_=i)

    sibling = at(c_=1 - c)

    barrier = pltpu.get_barrier_semaphore()

    def greet(device):
        pl.semaphore_signal(barrier, inc=1, device_id=device, device_id_type=MESH)

    @pl.loop(0, 16)
    def _(i):
        t = lax.rem(x * 4 + zl + i, 16)
        greet(at(x_=t // 4, zl_=lax.rem(t, 4), zh_=1 - zh))

    @pl.loop(1, 32)
    def _(i):
        t = lax.rem(clip + i, 32)
        greet(at(x_=t // 8, zl_=lax.rem(t // 2, 4), c_=lax.rem(t, 2)))

    greet(at(c_=1 - c, zh_=1 - zh))
    for i in range(1, 4):
        greet(at(y_=lax.rem(y + i, 4)))
        greet(at(y_=lax.rem(y + i, 4), zh_=1 - zh))

    for half in range(2):
        for tile in range(100):
            rt, lt = half * 20 + tile // 5, tile % 5
            k = half * TILES + tile
            fin[k // PIECE, k % PIECE] = frames[8 * rt : 8 * rt + 8, 128 * lt : 128 * lt + 128]
        for tile in range(100, TILES):
            k = half * TILES + tile
            fin[k // PIECE, k % PIECE] = jnp.zeros((8, 128), BF16)
    for h in range(2):
        tail[h, 0:4] = out_in[:, 640 * h : 640 * h + 640]
        tail[h, 4:24] = fc2_in[:, 640 * h : 640 * h + 640]
    for t in range(3):
        wq[zh, x, zl, c, :, 128 * t : 128 * t + 128] = qkv_in[:, t, :]
    bias[0:1, :] = b_fc1[...]
    bias[1:2, 0:160] = b_out[...]
    bias[2:3, 0:160] = b_fc2[...]
    bias[3:5, 0:128] = b_qv[...]
    own_1 = pltpu.make_async_copy(fc1_in, w1.at[zh, x, zl, c], local.at[0])
    own_1.start()

    zq = Ring8(lambda i: wq.at[i // 4, x, lax.rem(i, 4), c], z, at_z, s_zq, r_zq)
    zo = Ring8(lambda i: wo.at[c, y, i // 4, x, lax.rem(i, 4)], z, at_z, s_zo, r_zo)
    z1 = Ring8(lambda i: w1.at[i // 4, x, lax.rem(i, 4), c], z, at_z, s_z1, r_z1)
    z2 = Ring8(lambda i: w2.at[c, i // 4, :, lax.rem(i, 4)], z, at_z, s_z2, r_z2)
    xq = Ring4(lambda i: wq.at[:, i, :, c], lambda i, h: wq.at[h, i, :, c], x, at_x, s_xq, r_xq)
    xo = Ring4(lambda i: wo.at[c, y, :, i], lambda i, h: wo.at[c, y, h, i], x, at_x, s_xo, r_xo)
    x1 = Ring4(lambda i: w1.at[:, i, :, c], lambda i, h: w1.at[h, i, :, c], x, at_x, s_x1, r_x1)
    x2 = Ring4(
        lambda i: w2.at[c, zh, i, zl],
        lambda i, h: w2.at[c, zh, i, zl, pl.ds(24 * h, 24 - 8 * h)],
        x, at_x, s_x2, r_x2,
    )
    yo = Ring4(lambda i: wo.at[c, i], lambda i, h: wo.at[c, i, h], y, at_y, s_yo, r_yo)

    def yx(t):
        tiles = pl.ds(t * 20, 20)
        return Ring4(
            lambda i: xg.at[i, :, tiles], lambda i, h: xg.at[i, h, tiles], y, at_y, s_yx, r_yx, t * 4
        )

    def yn(t):
        def rows(first, count):
            return pl.ds(pl.multiple_of(t * ROWS + first, 16), count)

        return Ring4(
            lambda i: n2.at[i, rows(0, ROWS)], lambda i, h: n2.at[i, rows(16 * h, 16)],
            y, at_y, s_yn, r_yn, t * 4,
        )

    dq = remote(wq.at[:, :, :, c], wq.at[:, :, :, c], s_d.at[0], r_d.at[0], sibling)
    d1 = remote(w1.at[:, :, :, c], w1.at[:, :, :, c], s_d.at[1], r_d.at[1], sibling)
    d2 = remote(w2.at[c], w2.at[c], s_d.at[2], r_d.at[2], sibling)
    dkv = remote(kv.at[c], kv.at[c], s_d.at[3], r_d.at[3], sibling)
    do = []
    for n in range(4):
        part = wo.at[c, lax.rem(y + (0, 1, 3, 2)[n], 4)]
        do.append(remote(part, part, s_d.at[4 + n], r_d.at[4 + n], sibling))
    bias_sends = []
    for i in range(4):
        for other in range(2):
            if i or other:
                device = at(y_=lax.rem(y + i, 4), zh_=(1 - zh) if other else zh)
                n = i * 2 + other
                bias_sends.append(
                    remote(bias, bg.at[y * 2 + zh], s_bias.at[n], r_bias.at[n], device)
                )
    own_b = pltpu.make_async_copy(bias, bg.at[y * 2 + zh], local.at[1])
    own_pair = pltpu.make_async_copy(tail.at[c], pair.at[c], local.at[2])
    to_pair = remote(tail.at[1 - c], pair.at[c], s_pair, r_pair, sibling)

    pl.semaphore_wait(barrier, 54)

    to_pair.start()
    zq.start(0)
    own_b.start()
    own_pair.start()

    def piece_of(x_, zl_, c_):
        return c_ * 16 + x_ * 4 + zl_

    def regroup_sends(first, last):
        @pl.loop(first, last)
        def _(i):
            t = lax.rem(clip + i, 32)
            x_, zl_, c_ = t // 8, lax.rem(t // 2, 4), lax.rem(t, 2)
            remote(
                fin.at[piece_of(x_, zl_, c_)], p1.at[clip], s_p1, r_p1, at(x_=x_, zl_=zl_, c_=c_)
            ).start()

    keep_one = pltpu.make_async_copy(fin.at[piece_of(x, zl, c)], p1.at[clip], r_p1)
    keep_one.start()
    regroup_sends(1, 9)
    own_pair.wait()
    to_pair.wait_recv()
    wo[c, y, zh, x, zl, 0:4] = pair[0, 0:4]
    wo[c, y, zh, x, zl, 4:8] = pair[1, 0:4]
    w2[c, zh, x, zl, 0:20] = pair[0, 4:24]
    w2[c, zh, x, zl, 20:40] = pair[1, 4:24]
    zo.start(0)
    zq.relay(0)
    regroup_sends(9, 17)
    zo.relay(0)
    zq.relay(1)
    regroup_sends(17, 25)
    zo.relay(1)
    zq.relay(2)
    regroup_sends(25, 32)
    zo.relay(2)
    x2.start()
    for copy in bias_sends:
        copy.start()
    zq.arrive(3)
    xq.start()
    own_1.wait()
    own_b.wait()

    pltpu.make_async_copy(p1, p1, r_p1).wait()

    @pl.loop(0, 32)
    def _(s):
        p2[s] = p1[order[s]]

    slot = x * 8 + zl * 2 + zh
    place = xg.at[y, zh, pl.ds(PIECE * (x * 4 + zl), PIECE)]

    @pl.loop(1, 32)
    def _(i):
        t = lax.rem(slot + i, 32)
        remote(
            p2.at[t], place, s_p2, r_p2, at(x_=t // 8, zl_=lax.rem(t // 2, 4), zh_=lax.rem(t, 2))
        ).start()

    keep_two = pltpu.make_async_copy(p2.at[slot], place, r_p2)
    keep_two.start()

    z1.start(0)
    x2.forward()
    zo.arrive(3)
    xo.start()
    xq.forward()
    xo.forward()
    x2.arrive()
    z2.start(0)
    xq.arrive()
    dq.start()
    pltpu.make_async_copy(xg.at[y], xg.at[y], r_p2).wait()

    yx(0).start()
    yx(1).start()
    z1.relay(0)
    for copy in bias_sends:
        copy.wait_recv()
    yx(0).forward()
    yx(2).start()
    dq.wait_recv()

    def project(t):
        @pl.loop(0, 2)
        def _(u):
            first = t * 20 + u * 10
            blocks = []
            for b in range(8):
                parts = [
                    jnp.concatenate(
                        [xg[b // 2, b % 2, first + lt], xg[b // 2, b % 2, first + 5 + lt]], axis=0
                    )
                    for lt in range(5)
                ]
                blocks.append(jnp.concatenate(parts, axis=1))
            start = pl.multiple_of(t * ROWS + u * 16, 16)
            inner = pl.multiple_of(u * 16, 16)
            for j in range(4):
                whole = jnp.concatenate(
                    [block[:, 160 * j : 160 * j + 160] for block in blocks], axis=1
                )
                xr[j, pl.ds(start, 16)] = whole
                xn[j, pl.ds(inner, 16)] = layer_norm(whole.astype(F32), g1[...], s1[...])

        left = xn[...].reshape(4 * ROWS, D)
        for h in range(2):
            prod = dot(left, wq[h].reshape(D, 384))
            biases = bg[y * 2 + h]
            lanes = slice(128 * h, 128 * h + 128)
            query = ((prod[:, 0:128] + biases[3:4, 0:128]) * HDIM ** (-0.5)).astype(BF16)
            key = prod[:, 128:256].astype(BF16)
            value = (prod[:, 256:384] + biases[4:5, 0:128]).astype(BF16)
            for j in range(4):
                rows = pl.ds(pl.multiple_of(j * HALF + t * ROWS, 16), ROWS)
                part = slice(ROWS * j, ROWS * j + ROWS)
                qs[rows, lanes] = query[part]
                kv[c, 0, rows, lanes] = key[part]
                kv[c, 1, rows, lanes] = value[part]

    @pl.loop(0, CHUNKS)
    def _(t):
        @pl.when(t < CHUNKS - 1)
        def _():
            yx(t + 1).forward()

        @pl.when(t < CHUNKS - 3)
        def _():
            yx(t + 3).start()

        for n in range(3):
            @pl.when(t == n)
            def _():
                z1.relay(n + 1)

        @pl.when(t == 2)
        def _():
            z2.relay(0)

        yx(t).arrive()
        project(t)

    dkv.start()
    x1.start()
    xo.arrive()
    yo.start()
    do[0].start()
    z2.relay(1)
    dkv.wait_recv()

    head_of = lax.broadcasted_iota(jnp.int32, (HALF, 256), 1) // HDIM

    def attend(j):
        rows = pl.ds(pl.multiple_of(j * HALF, HALF), HALF)
        q = qs[rows, :]
        zero = jnp.zeros_like(q)
        stacked = jnp.concatenate([jnp.where(head_of == h, q, zero) for h in range(4)], axis=0)
        keys = kv[:, 0].reshape(D, 256)
        scores = lax.dot_general(
            stacked, keys, (((1,), (1,)), ((), ())), preferred_element_type=F32
        )
        weights = jnp.exp(scores - jnp.max(scores, axis=-1, keepdims=True))
        total = jnp.sum(weights, axis=-1, keepdims=True)
        mixed = dot(weights.astype(BF16), kv[:, 1].reshape(D, 256)) / total
        context = jnp.zeros((HALF, 256), F32)
        for h in range(4):
            context = context + jnp.where(head_of == h, mixed[h * HALF : (h + 1) * HALF], 0.0)
        return context.astype(BF16)

    @pl.loop(1, 4)
    def _(i):
        j = lax.rem(y + i, 4)
        cx[4 + j] = attend(j)
        remote(cx.at[4 + j], cx.at[y], s_cx.at[i - 1], r_cx.at[i - 1], at(y_=j)).start()

        @pl.when(i == 1)
        def _():
            z2.relay(2)

        @pl.when(i == 2)
        def _():
            yo.forward()
            do[1].start()
            do[2].start()

    x1.forward()
    z2.arrive(3)
    d2.start()
    cx[y] = attend(y)
    yo.arrive()
    do[3].start()
    x1.arrive()
    d1.start()
    for i in range(1, 4):
        remote(cx.at[0], cx.at[0], s_cx.at[i - 1], r_cx.at[i - 1], sibling).wait_recv()
    for copy in do:
        copy.wait_recv()

    def whole_bias(row):
        return jnp.concatenate([bg[h, row : row + 1, 0:160] for h in range(8)], axis=1)

    context = jnp.concatenate([cx[i] for i in range(4)], axis=1)
    product = jnp.concatenate(
        [dot(context, wo[h].reshape(1024, 640)) for h in range(2)], axis=1
    )
    attended = (xr[y].astype(F32) + whole_bias(1) + product).astype(BF16)
    att[...] = attended.astype(F32) + whole_bias(2)
    n2[y] = layer_norm(attended.astype(F32), g2[...], s2[...])
    yn(0).start()
    yn(1).start()
    yn(0).forward()
    yn(2).start()
    d1.wait_recv()
    d2.wait_recv()

    up, down, far = lax.rem(y + 1, 4), lax.rem(y + 3, 4), lax.rem(y + 2, 4)

    def rows_of(t):
        return pl.ds(pl.multiple_of(t * ROWS, ROWS), ROWS)

    def sums(t):
        r, n = rows_of(t), 4 * t
        return [
            remote(pk.at[far, 0, r], ra.at[r], s_rs.at[n], r_rs.at[n], at(y_=up)),
            remote(pk.at[far, 1, r], rb.at[r], s_rs.at[n + 1], r_rs.at[n + 1], at(y_=down)),
            remote(pk.at[up, :, r], rc.at[:, r], s_rs.at[n + 2], r_rs.at[n + 2], at(y_=up)),
            remote(pk.at[down, :, r], rd.at[:, r], s_rs.at[n + 3], r_rs.at[n + 3], at(y_=down)),
        ]

    def feed_forward(t):
        r = rows_of(t)
        left = jnp.concatenate([n2[j, r] for j in range(4)], axis=0)
        parts = []
        for h in range(2):
            total = dot(left, w1[h].reshape(D, 640)) + bg[y * 2 + h, 0:1, :]
            parts.append((0.5 * total * (1.0 + lax.erf(total * 0.5**0.5))).astype(BF16))
        hidden = jnp.concatenate(parts, axis=1)
        share = jnp.concatenate(
            [dot(hidden, w2[h].reshape(D, 640)) for h in range(2)], axis=1
        )
        kept = att[r]
        for j in range(4):
            part = share[ROWS * j : ROWS * j + ROWS] + jnp.where(y == j, kept, 0.0)
            for b in range(8):
                pk[b // 2, b % 2, r, 160 * j : 160 * j + 160] = part[
                    :, 160 * b : 160 * b + 160
                ].astype(BF16)
        sums(t)[0].start()
        sums(t)[1].start()

    def add_and_pass(t):
        r = rows_of(t)
        copies = sums(t)
        copies[0].wait_recv()
        pk[up, 0, r] = (pk[up, 0, r].astype(F32) + ra[r].astype(F32)).astype(BF16)
        copies[2].start()
        copies[1].wait_recv()
        pk[down, 1, r] = (pk[down, 1, r].astype(F32) + rb[r].astype(F32)).astype(BF16)
        copies[3].start()

    def out_rows(t):
        return out.at[pl.ds(pl.multiple_of(c * HALF + t * ROWS, ROWS), ROWS)]

    def finish(t):
        r = rows_of(t)
        copies = sums(t)
        copies[2].wait_recv()
        copies[3].wait_recv()
        fo[:, r] = (pk[y, :, r].astype(F32) + rc[:, r].astype(F32) + rd[:, r].astype(F32)).astype(
            BF16
        )
        remote(fo.at[1 - zh, r], out_rows(t), s_out, r_out, at(c_=zh, zh_=1 - zh)).start()

        @pl.when(c == zh)
        def _():
            pltpu.make_async_copy(fo.at[zh, r], out_rows(t), r_out).start()

        @pl.when(c != zh)
        def _():
            remote(fo.at[zh, r], out_rows(t), s_next, r_out, sibling).start()

    @pl.loop(0, CHUNKS)
    def _(t):
        @pl.when(t < CHUNKS - 1)
        def _():
            yn(t + 1).forward()

        @pl.when(t < CHUNKS - 3)
        def _():
            yn(t + 3).start()

        yn(t).arrive()
        feed_forward(t)

        @pl.when(t > 0)
        def _():
            add_and_pass(t - 1)

        @pl.when(t > 1)
        def _():
            finish(t - 2)

    add_and_pass(CHUNKS - 1)
    finish(CHUNKS - 2)
    finish(CHUNKS - 1)

    pltpu.make_async_copy(out, out, r_out).wait()

    pltpu.make_async_copy(fo.at[0], fo.at[0], s_out).wait()

    @pl.when(c != zh)
    def _():
        pltpu.make_async_copy(fo.at[0], fo.at[0], s_next).wait()

    to_pair.wait_send()
    pltpu.make_async_copy(p1.at[pl.ds(0, 31)], p1.at[pl.ds(0, 31)], s_p1).wait()
    pltpu.make_async_copy(p1.at[pl.ds(0, 31)], p1.at[pl.ds(0, 31)], s_p2).wait()
    for copy in bias_sends + do + [dq, d1, d2, dkv]:
        copy.wait_send()
    for i in range(1, 4):
        remote(cx.at[0], cx.at[0], s_cx.at[i - 1], r_cx.at[i - 1], sibling).wait_send()
    for ring in (zq, zo, z1, z2, xq, xo, x1, x2, yo):
        ring.drain()

    @pl.loop(0, CHUNKS)
    def _(t):
        yx(t).drain()
        yn(t).drain()
        for copy in sums(t):
            copy.wait_send()


def slot_order(server_list):
    clip_count = server_list.shape[0]
    indices = jnp.arange(clip_count, dtype=jnp.int32)
    earlier = (server_list[None, :] < server_list[:, None]) | (
        server_list[None, :] == server_list[:, None]
    ) & (indices[None, :] < indices[:, None])
    slot_of = jnp.sum(earlier.astype(jnp.int32), axis=1)
    return jnp.sum(jnp.where(slot_of[None, :] == indices[:, None], indices[None, :], 0), axis=1)


def on_device(
    frames_in, ln1_gain, ln1_bias, qkv_weight, qv_bias, out_weight, out_bias,
    ln2_gain, ln2_bias, fc1_weight, fc1_bias, fc2_weight, fc2_bias, server_of_clip,
):
    clip_order = slot_order(server_of_clip)
    vmem = pl.BlockSpec(memory_space=pltpu.VMEM)
    smem = pl.BlockSpec(memory_space=pltpu.SMEM)
    dma = pltpu.SemaphoreType.DMA
    V = pltpu.VMEM
    out = pl.pallas_call(
        kernel,
        out_shape=jax.ShapeDtypeStruct((320, 640), BF16),
        in_specs=[smem] + [vmem] * 13,
        out_specs=vmem,
        scratch_shapes=[
            V((32, PIECE, 8, 128), BF16),
            V((32, PIECE, 8, 128), BF16),
            V((32, PIECE, 8, 128), BF16),
            V((4, 2, TILES, 8, 128), BF16),
            V((2, 4, 4, 2, 40, 384), BF16),
            V((2, 4, 4, 2, 40, 640), BF16),
            V((2, 2, 4, 4, 40, 640), BF16),
            V((2, 4, 2, 4, 4, 8, 640), BF16),
            V((2, 24, 640), BF16),
            V((2, 24, 640), BF16),
            V((8, 640), F32),
            V((8, 8, 640), F32),
            V((4, HALF, D), BF16),
            V((4, ROWS, D), BF16),
            V((640, 256), BF16),
            V((2, 2, 640, 256), BF16),
            V((8, HALF, 256), BF16),
            V((HALF, D), F32),
            V((4, HALF, D), BF16),
            V((4, 2, HALF, 640), BF16),
            V((HALF, 640), BF16),
            V((HALF, 640), BF16),
            V((2, HALF, 640), BF16),
            V((2, HALF, 640), BF16),
            V((2, HALF, 640), BF16),
            dma((3,)),
            dma, dma, dma, dma, dma, dma, dma((8,)), dma((8,)),
            dma((7,)), dma((7,)), dma((7,)), dma((7,)), dma((7,)), dma((7,)), dma((7,)), dma((7,)),
            dma((4,)), dma((4,)), dma((4,)), dma((4,)), dma((4,)), dma((4,)), dma((4,)), dma((4,)),
            dma((4 * CHUNKS,)), dma((4 * CHUNKS,)), dma((4,)), dma((4,)),
            dma((4 * CHUNKS,)), dma((4 * CHUNKS,)),
            dma((8,)), dma((8,)), dma((3,)), dma((3,)), dma((4 * CHUNKS,)), dma((4 * CHUNKS,)),
            dma, dma, dma,
        ],
        compiler_params=pltpu.CompilerParams(
            collective_id=0, has_side_effects=True, vmem_limit_bytes=60 * 2**20
        ),
    )(
        clip_order, frames_in.reshape(320, 640), qkv_weight, fc1_weight, out_weight, fc2_weight,
        qv_bias, out_bias[None], fc1_bias[None], fc2_bias[None],
        ln1_gain[None], ln1_bias[None], ln2_gain[None], ln2_bias[None],
    )
    return out.reshape(1, 1, 320, 640)


def solution(mesh):
    torus = Mesh(mesh.devices.reshape(4, 4, 2, 4, 2), ("x", "zl", "c", "y", "zh"))
    return jax.shard_map(
        on_device,
        mesh=torus,
        in_specs=(
            P(DP, HEAD, None, None), P(), P(), P(DP, None, HEAD), P(None, HEAD), P(HEAD_DP, None),
            P(HEAD), P(), P(), P(DP, HEAD), P(HEAD), P(HEAD_DP, None), P(HEAD), P(),
        ),
        out_specs=P(DP, HEAD, None, None),
        check_vma=False,
    )
```

```python
import functools

import jax
import jax.numpy as jnp
from jax import lax
from jax.experimental import pallas as pl
from jax.experimental.pallas import tpu as pltpu
from jax.sharding import Mesh
from jax.sharding import PartitionSpec as P

MESH = pl.DeviceIdType.MESH
BF16 = jnp.bfloat16
F32 = jnp.float32
EPS = 1e-05
HDIM = 64
DP = ("x", "zl", "c")
HEAD = ("y", "zh")
HEAD_DP = ("y", "zh", "x", "zl", "c")

D = 1280
HALF = 160
TILES = 100
PIECE = 6
CHUNKS = 5
ROWS = 32


def remote(src, dst, send, recv, device):
    return pltpu.make_async_remote_copy(
        src_ref=src, dst_ref=dst, send_sem=send, recv_sem=recv,
        device_id=device, device_id_type=MESH,
    )


class Ring4:
    def __init__(self, slab, half, i, device, send, recv, base=0):
        up, down = lax.rem(i + 1, 4), lax.rem(i + 3, 4)
        own = slab(i)

        def sems(n):
            return send.at[base + n], recv.at[base + n]

        self.one = [
            remote(own, own, *sems(0), device(up)),
            remote(own, own, *sems(1), device(down)),
        ]
        self.two = [
            remote(half(down, 0), half(down, 0), *sems(2), device(up)),
            remote(half(up, 1), half(up, 1), *sems(3), device(down)),
        ]

    def start(self):
        for copy in self.one:
            copy.start()

    def forward(self):
        for copy, nxt in zip(self.one, self.two):
            copy.wait_recv()
            nxt.start()

    def arrive(self):
        for copy in self.two:
            copy.wait_recv()

    def drain(self):
        for copy in self.one + self.two:
            copy.wait_send()


class Ring8:
    def __init__(self, slab, i, device, send, recv):
        up, down = lax.rem(i + 1, 8), lax.rem(i + 7, 8)
        self.steps = []
        for s in range(4):
            older = slab(lax.rem(i + 8 - s, 8))
            copies = [remote(older, older, send.at[2 * s], recv.at[2 * s], device(up))]
            if s < 3:
                newer = slab(lax.rem(i + s, 8))
                copies.append(
                    remote(newer, newer, send.at[2 * s + 1], recv.at[2 * s + 1], device(down))
                )
            self.steps.append(copies)

    def start(self, s):
        for copy in self.steps[s]:
            copy.start()

    def arrive(self, s):
        for copy in self.steps[s]:
            copy.wait_recv()

    def relay(self, s):
        self.arrive(s)
        if s < 3:
            self.start(s + 1)

    def drain(self):
        for copies in self.steps:
            for copy in copies:
                copy.wait_send()


def layer_norm(floats, gain, shift):
    center = jnp.sum(floats, axis=-1, keepdims=True) * (1.0 / D)
    moved = floats - center
    spread = jnp.sum(moved * moved, axis=-1, keepdims=True) * (1.0 / D)
    return (moved * lax.rsqrt(spread + EPS) * gain + shift).astype(BF16)


def dot(a, b):
    return jnp.dot(a, b, preferred_element_type=F32)


def kernel(
    servers, frames_hbm, qkv_hbm, fc1_in, out_hbm, fc2_hbm, qv_hbm, bo_hbm, b1_hbm, b2_hbm,
    g1_hbm, s1_hbm, g2_hbm, s2_hbm,
    out,
    keys, slots, order, frames, qkv_in, out_in, fc2_in, b_qv, b_out, b_fc1, b_fc2, g1, s1, g2, s2,
    norms, fin, p1, p2, xg, wq, w1, w2, wo, tail, pair, bias, bg, xr, xn, qs, kv, cs, cx, att, n2, pk,
    ra, rb, rc, rd, fo,
    fetch, local, s_p1, r_p1, s_p2, r_p2, s_more, r_more, s_last, s_pair, r_pair, s_bias, r_bias,
    s_zq, r_zq, s_zo, r_zo, s_z1, r_z1, s_z2, r_z2,
    s_xq, r_xq, s_xo, r_xo, s_x1, r_x1, s_x2, r_x2,
    s_yx, r_yx, s_yo, r_yo, s_yn, r_yn, s_d, r_d, s_kv, r_kv, s_cx, r_cx, s_rs, r_rs, s_out, s_next, r_out,
):
    x, zl, c = lax.axis_index("x"), lax.axis_index("zl"), lax.axis_index("c")
    y, zh = lax.axis_index("y"), lax.axis_index("zh")
    z = zh * 4 + zl
    clip = x * 8 + zl * 2 + c

    def at(x_=x, zl_=zl, c_=c, y_=y, zh_=zh):
        return (x_, zl_, c_, y_, zh_)

    def at_z(z_):
        return at(zl_=lax.rem(z_, 4), zh_=z_ // 4)

    def at_x(i):
        return at(x_=i)

    def at_y(i):
        return at(y_=i)

    sibling = at(c_=1 - c)

    fetches = [
        pltpu.make_async_copy(src, dst, fetch.at[n])
        for n, (src, dst) in enumerate(
            [(frames_hbm, frames), (out_hbm, out_in), (fc2_hbm, fc2_in), (qkv_hbm, qkv_in),
             (qv_hbm, b_qv), (bo_hbm, b_out), (b1_hbm, b_fc1), (b2_hbm, b_fc2), (g1_hbm, g1),
             (s1_hbm, s1), (g2_hbm, g2), (s2_hbm, s2), (fc1_in, w1.at[zh, x, zl, c])]
        )
    ]
    for copy in fetches:
        copy.start()
    barrier = pltpu.get_barrier_semaphore()

    def greet(device):
        pl.semaphore_signal(barrier, inc=1, device_id=device, device_id_type=MESH)

    @pl.loop(0, 16)
    def _(i):
        t = lax.rem(x * 4 + zl + i, 16)
        greet(at(x_=t // 4, zl_=lax.rem(t, 4), zh_=1 - zh))

    @pl.loop(1, 32)
    def _(i):
        t = lax.rem(clip + i, 32)
        greet(at(x_=t // 8, zl_=lax.rem(t // 2, 4), c_=lax.rem(t, 2)))

    greet(at(c_=1 - c, zh_=1 - zh))
    for i in range(1, 4):
        greet(at(y_=lax.rem(y + i, 4)))
        greet(at(y_=lax.rem(y + i, 4), zh_=1 - zh))

    for copy in fetches:
        copy.wait()

    for half in range(2):
        for tile in range(100):
            rt, lt = half * 20 + tile // 5, tile % 5
            fin[half, tile] = frames[8 * rt : 8 * rt + 8, 128 * lt : 128 * lt + 128]
    for h in range(2):
        tail[h, 0:4] = out_in[:, 640 * h : 640 * h + 640]
        tail[h, 4:24] = fc2_in[:, 640 * h : 640 * h + 640]
    for t in range(3):
        wq[zh, x, zl, c, :, 128 * t : 128 * t + 128] = qkv_in[t]
    def flat(ref):
        return jnp.concatenate([ref[i : i + 1] for i in range(ref.shape[0])], axis=1)

    bias[0:1, :] = flat(b_fc1)
    for i, ref in enumerate((g1, s1, g2, s2)):
        norms[i : i + 1] = flat(ref)
    bias[1:2, 0:160] = b_out[...]
    bias[2:3, 0:160] = b_fc2[...]
    bias[3:5, 0:128] = b_qv[...]

    zq = Ring8(lambda i: wq.at[i // 4, x, lax.rem(i, 4), c], z, at_z, s_zq, r_zq)
    zo = Ring8(lambda i: wo.at[c, y, i // 4, x, lax.rem(i, 4)], z, at_z, s_zo, r_zo)
    z1 = Ring8(lambda i: w1.at[i // 4, x, lax.rem(i, 4), c], z, at_z, s_z1, r_z1)
    z2 = Ring8(lambda i: w2.at[c, i // 4, :, lax.rem(i, 4)], z, at_z, s_z2, r_z2)
    xq = Ring4(lambda i: wq.at[:, i, :, c], lambda i, h: wq.at[h, i, :, c], x, at_x, s_xq, r_xq)
    xo = Ring4(lambda i: wo.at[c, y, :, i], lambda i, h: wo.at[c, y, h, i], x, at_x, s_xo, r_xo)
    x1 = Ring4(lambda i: w1.at[:, i, :, c], lambda i, h: w1.at[h, i, :, c], x, at_x, s_x1, r_x1)
    x2 = Ring4(
        lambda i: w2.at[c, zh, i, zl],
        lambda i, h: w2.at[c, zh, i, zl, pl.ds(24 * h, 24 - 8 * h)],
        x, at_x, s_x2, r_x2,
    )
    yo = Ring4(lambda i: wo.at[c, i], lambda i, h: wo.at[c, i, h], y, at_y, s_yo, r_yo)

    def yx(t):
        tiles = pl.ds(t * 20, 20)
        return Ring4(
            lambda i: xg.at[i, :, tiles], lambda i, h: xg.at[i, h, tiles], y, at_y, s_yx, r_yx, t * 4
        )

    def yn(t):
        def rows(first, count):
            return pl.ds(pl.multiple_of(t * ROWS + first, 16), count)

        return Ring4(
            lambda i: n2.at[i, rows(0, ROWS)], lambda i, h: n2.at[i, rows(16 * h, 16)],
            y, at_y, s_yn, r_yn, t * 4,
        )

    dq = remote(wq.at[:, :, :, c], wq.at[:, :, :, c], s_d.at[0], r_d.at[0], sibling)
    d1 = remote(w1.at[:, :, :, c], w1.at[:, :, :, c], s_d.at[1], r_d.at[1], sibling)
    d2 = remote(w2.at[c], w2.at[c], s_d.at[2], r_d.at[2], sibling)

    def dkv(t):
        return remote(kv.at[c, t], kv.at[c, t], s_kv.at[t], r_kv.at[t], sibling)

    do = []
    for n in range(4):
        part = wo.at[c, lax.rem(y + (0, 1, 3, 2)[n], 4)]
        do.append(remote(part, part, s_d.at[3 + n], r_d.at[3 + n], sibling))
    bias_sends = []
    for i in range(4):
        for other in range(2):
            if i or other:
                device = at(y_=lax.rem(y + i, 4), zh_=(1 - zh) if other else zh)
                n = i * 2 + other
                bias_sends.append(
                    remote(bias, bg.at[y * 2 + zh], s_bias.at[n], r_bias.at[n], device)
                )
    own_b = pltpu.make_async_copy(bias, bg.at[y * 2 + zh], local.at[1])
    own_pair = pltpu.make_async_copy(tail.at[c], pair.at[c], local.at[2])
    to_pair = remote(tail.at[1 - c], pair.at[c], s_pair, r_pair, sibling)

    pl.semaphore_wait(barrier, 54)

    to_pair.start()
    zq.start(0)
    own_b.start()
    own_pair.start()

    def first_tile(x_, zl_):
        return x_ * 25 + zl_ * PIECE + jnp.minimum(zl_, 1)

    def regroup_sends(first, last):
        @pl.loop(first, last)
        def _(i):
            t = lax.rem(clip + i, 32)
            x_, zl_, c_ = t // 8, lax.rem(t // 2, 4), lax.rem(t, 2)
            tile = first_tile(x_, zl_)
            device = at(x_=x_, zl_=zl_, c_=c_)
            remote(
                fin.at[c_, pl.ds(tile, PIECE)], p1.at[clip, pl.ds(0, PIECE)], s_p1, r_p1, device
            ).start()

            @pl.when(zl_ == 0)
            def _():
                remote(
                    fin.at[c_, tile + PIECE], p1.at[clip, PIECE], s_more, r_more, device
                ).start()

    own_tile = first_tile(x, zl)
    keep_one = pltpu.make_async_copy(
        fin.at[c, pl.ds(own_tile, PIECE)], p1.at[clip, pl.ds(0, PIECE)], r_p1
    )
    keep_one.start()
    keep_more = pltpu.make_async_copy(fin.at[c, own_tile + PIECE], p1.at[clip, PIECE], r_more)

    @pl.when(zl == 0)
    def _():
        keep_more.start()

    regroup_sends(1, 12)
    own_pair.wait()
    to_pair.wait_recv()
    wo[c, y, zh, x, zl, 0:4] = pair[0, 0:4]
    wo[c, y, zh, x, zl, 4:8] = pair[1, 0:4]
    w2[c, zh, x, zl, 0:20] = pair[0, 4:24]
    w2[c, zh, x, zl, 20:40] = pair[1, 4:24]

    for i in range(32):
        keys[i] = servers[i] * 32 + i

    def count_smaller(first, last):
        @pl.loop(first, last)
        def _(i):
            own, total = keys[i], jnp.int32(0)
            for other in range(32):
                total = total + jnp.where(keys[other] < own, 1, 0)
            slots[i] = total

    count_smaller(0, 10)
    zq.relay(0)
    regroup_sends(12, 22)
    count_smaller(10, 21)
    zq.relay(1)
    regroup_sends(22, 32)
    x2.start()
    count_smaller(21, 32)
    zq.relay(2)

    @pl.loop(0, 32)
    def _(i):
        total = jnp.int32(0)
        for other in range(32):
            total = total + jnp.where(slots[other] == i, other, 0)
        order[i] = total

    own_b.wait()
    zq.arrive(3)
    xq.start()

    most = p1.at[:, pl.ds(0, PIECE)]
    pltpu.make_async_copy(most, most, r_p1).wait()

    @pl.when(zl == 0)
    def _():
        pltpu.make_async_copy(p1.at[:, PIECE], p1.at[:, PIECE], r_more).wait()

    @pl.loop(0, 32)
    def _(s):
        p2[s, 0:PIECE] = p1[order[s], 0:PIECE]

    @pl.when(zl == 0)
    def _():
        @pl.loop(0, 32)
        def _(s):
            p2[s, PIECE] = p1[order[s], PIECE]

    slot = x * 8 + zl * 2 + zh
    place = xg.at[y, zh, pl.ds(own_tile, PIECE)]
    place_more = xg.at[y, zh, own_tile + PIECE]

    @pl.loop(1, 32)
    def _(i):
        t = lax.rem(slot + i, 32)
        device = at(x_=t // 8, zl_=lax.rem(t // 2, 4), zh_=lax.rem(t, 2))
        remote(p2.at[t, pl.ds(0, PIECE)], place, s_p2, r_p2, device).start()

        @pl.when(zl == 0)
        def _():
            remote(p2.at[t, PIECE], place_more, s_last, r_p2, device).start()

    keep_two = pltpu.make_async_copy(p2.at[slot, pl.ds(0, PIECE)], place, r_p2)
    keep_two.start()
    keep_last = pltpu.make_async_copy(p2.at[slot, PIECE], place_more, r_p2)

    @pl.when(zl == 0)
    def _():
        keep_last.start()

    x2.forward()
    zo.start(0)
    z1.start(0)
    for copy in bias_sends:
        copy.start()
    xq.forward()
    zo.relay(0)
    pltpu.make_async_copy(xg.at[y], xg.at[y], r_p2).wait()

    yx(0).start()
    yx(1).start()
    xq.arrive()
    dq.start()
    zo.relay(1)
    z1.relay(0)
    yx(0).forward()
    yx(2).start()
    zo.relay(2)
    for copy in bias_sends:
        copy.wait_recv()
    x2.arrive()
    dq.wait_recv()

    def project(t):
        @pl.loop(0, 2)
        def _(u):
            first = t * 20 + u * 10
            blocks = []
            for b in range(8):
                parts = [
                    jnp.concatenate(
                        [xg[b // 2, b % 2, first + lt], xg[b // 2, b % 2, first + 5 + lt]], axis=0
                    )
                    for lt in range(5)
                ]
                blocks.append(jnp.concatenate(parts, axis=1))
            start = pl.multiple_of(t * ROWS + u * 16, 16)
            inner = pl.multiple_of(u * 16, 16)
            for j in range(4):
                whole = jnp.concatenate(
                    [block[:, 160 * j : 160 * j + 160] for block in blocks], axis=1
                )
                xr[j, pl.ds(start, 16)] = whole
                xn[j, pl.ds(inner, 16)] = layer_norm(whole.astype(F32), norms[0:1], norms[1:2])

        left = xn[...].reshape(4 * ROWS, D)
        for h in range(2):
            prod = dot(left, wq[h].reshape(D, 384))
            biases = bg[y * 2 + h]
            lanes = slice(128 * h, 128 * h + 128)
            query = ((prod[:, 0:128] + biases[3:4, 0:128]) * HDIM ** (-0.5)).astype(BF16)
            key = prod[:, 128:256].astype(BF16)
            value = (prod[:, 256:384] + biases[4:5, 0:128]).astype(BF16)
            qs[t, :, lanes] = query
            kv[c, t, 0, :, lanes] = key
            kv[c, t, 1, :, lanes] = value
        dkv(t).start()

    @pl.loop(0, CHUNKS)
    def _(t):
        with jax.named_scope("L_fwd"):
            @pl.when(t < CHUNKS - 1)
            def _():
                yx(t + 1).forward()

            @pl.when(t < CHUNKS - 3)
            def _():
                yx(t + 3).start()

        with jax.named_scope("L_z1"):
            @pl.when(t == 0)
            def _():
                zo.arrive(3)
                xo.start()
                z1.relay(1)

            @pl.when(t == 1)
            def _():
                z1.relay(2)

            @pl.when(t == 2)
            def _():
                xo.forward()
                z1.arrive(3)
                x1.start()
                z2.start(0)

            @pl.when(t == 4)
            def _():
                xo.arrive()
                yo.start()
                do[0].start()
                z2.relay(0)

        with jax.named_scope("L_arr"):
            yx(t).arrive()
        with jax.named_scope("L_proj"):
            project(t)

    for t in range(CHUNKS):
        dkv(t).wait_recv()

    head_of = lax.broadcasted_iota(jnp.int32, (4 * ROWS, 256), 1) // HDIM

    def rows_of(t):
        return pl.ds(pl.multiple_of(t * ROWS, ROWS), ROWS)

    def context_send(t, i):
        j = lax.rem(y + i, 4)
        n = 3 * t + i - 1
        return remote(cs.at[t, j], cx.at[y, rows_of(t)], s_cx.at[n], r_cx.at[n], at(y_=j))

    def attend(t):
        q = qs[t]
        zero = jnp.zeros_like(q)
        stacked = jnp.concatenate([jnp.where(head_of == h, q, zero) for h in range(4)], axis=0)
        keys = kv[:, :, 0].reshape(D, 256)
        scores = lax.dot_general(
            stacked, keys, (((1,), (1,)), ((), ())), preferred_element_type=F32
        )
        weights = jnp.exp(scores - jnp.max(scores, axis=-1, keepdims=True))
        total = jnp.sum(weights, axis=-1, keepdims=True)
        mixed = dot(weights.astype(BF16), kv[:, :, 1].reshape(D, 256)) / total
        context = jnp.zeros((4 * ROWS, 256), F32)
        for h in range(4):
            part = mixed[h * 4 * ROWS : (h + 1) * 4 * ROWS]
            context = context + jnp.where(head_of == h, part, 0.0)
        context = context.astype(BF16)
        for j in range(4):
            cs[t, j] = context[j * ROWS : (j + 1) * ROWS]
        for i in (2, 1, 3):
            context_send(t, i).start()
        cx[y, rows_of(t)] = cs[t, y]

    def whole_bias(row):
        return jnp.concatenate([bg[h, row : row + 1, 0:160] for h in range(8)], axis=1)

    def attend_out(t):
        r = rows_of(t)
        for i in range(1, 4):
            context_send(t, i).wait_recv()
        context = jnp.concatenate([cx[i, r] for i in range(4)], axis=1)
        product = jnp.concatenate(
            [dot(context, wo[h].reshape(1024, 640)) for h in range(2)], axis=1
        )
        attended = (xr[y, r].astype(F32) + whole_bias(1) + product).astype(BF16)
        att[r] = attended.astype(F32) + whole_bias(2)
        n2[y, r] = layer_norm(attended.astype(F32), norms[2:3], norms[3:4])
        yn(t).start()

    up, down, far = lax.rem(y + 1, 4), lax.rem(y + 3, 4), lax.rem(y + 2, 4)

    def sums(t):
        r, n = rows_of(t), 4 * t
        return [
            remote(pk.at[far, 0, r], ra.at[r], s_rs.at[n], r_rs.at[n], at(y_=up)),
            remote(pk.at[far, 1, r], rb.at[r], s_rs.at[n + 1], r_rs.at[n + 1], at(y_=down)),
            remote(pk.at[up, :, r], rc.at[:, r], s_rs.at[n + 2], r_rs.at[n + 2], at(y_=up)),
            remote(pk.at[down, :, r], rd.at[:, r], s_rs.at[n + 3], r_rs.at[n + 3], at(y_=down)),
        ]

    def feed_forward(t):
        r = rows_of(t)
        left = jnp.concatenate([n2[j, r] for j in range(4)], axis=0)
        parts = []
        for h in range(2):
            total = dot(left, w1[h].reshape(D, 640)) + bg[y * 2 + h, 0:1, :]
            parts.append((0.5 * total * (1.0 + lax.erf(total * 0.5**0.5))).astype(BF16))
        hidden = jnp.concatenate(parts, axis=1)
        share = jnp.concatenate(
            [dot(hidden, w2[h].reshape(D, 640)) for h in range(2)], axis=1
        )
        kept = att[r]
        for j in range(4):
            part = share[ROWS * j : ROWS * j + ROWS] + jnp.where(y == j, kept, 0.0)
            for b in range(8):
                pk[b // 2, b % 2, r, 160 * j : 160 * j + 160] = part[
                    :, 160 * b : 160 * b + 160
                ].astype(BF16)
        sums(t)[0].start()
        sums(t)[1].start()

    def add_and_pass(t):
        r = rows_of(t)
        copies = sums(t)
        copies[0].wait_recv()
        pk[up, 0, r] = (pk[up, 0, r].astype(F32) + ra[r].astype(F32)).astype(BF16)
        copies[2].start()
        copies[1].wait_recv()
        pk[down, 1, r] = (pk[down, 1, r].astype(F32) + rb[r].astype(F32)).astype(BF16)
        copies[3].start()

    def out_rows(t):
        return out.at[pl.ds(pl.multiple_of(c * HALF + t * ROWS, ROWS), ROWS)]

    def finish(t):
        r = rows_of(t)
        copies = sums(t)
        copies[2].wait_recv()
        copies[3].wait_recv()
        fo[:, r] = (pk[y, :, r].astype(F32) + rc[:, r].astype(F32) + rd[:, r].astype(F32)).astype(
            BF16
        )
        remote(fo.at[1 - zh, r], out_rows(t), s_out, r_out, at(c_=zh, zh_=1 - zh)).start()

        @pl.when(c == zh)
        def _():
            pltpu.make_async_copy(fo.at[zh, r], out_rows(t), r_out).start()

        @pl.when(c != zh)
        def _():
            remote(fo.at[zh, r], out_rows(t), s_next, r_out, sibling).start()

    def stage(name, i, lag, work):
        with jax.named_scope(name):
            @pl.when((i >= lag) & (i < lag + CHUNKS))
            def _():
                work(i - lag)

    def arrived(t):
        yn(t).arrive()

    @pl.loop(0, CHUNKS + 7)
    def _(i):
        stage("M_att", i, 0, attend)

        with jax.named_scope("M_w"):
            @pl.when(i == 0)
            def _():
                z2.relay(1)

            @pl.when(i == 1)
            def _():
                yo.forward()
                do[1].start()
                do[2].start()
                x1.forward()

            @pl.when(i == 2)
            def _():
                z2.relay(2)

            @pl.when(i == 3)
            def _():
                yo.arrive()
                do[3].start()
                x1.arrive()
                d1.start()
                for copy in do:
                    copy.wait_recv()

            @pl.when(i == 4)
            def _():
                z2.arrive(3)
                d2.start()

            @pl.when(i == 5)
            def _():
                d2.wait_recv()
                d1.wait_recv()

        stage("M_out", i, 3, attend_out)
        stage("M_fwd", i, 4, lambda t: yn(t).forward())
        stage("M_arr", i, 5, arrived)
        stage("M_ff", i, 5, feed_forward)
        stage("M_add", i, 6, add_and_pass)
        stage("M_fin", i, 7, finish)

    pltpu.make_async_copy(out, out, r_out).wait()

    pltpu.make_async_copy(fo.at[0], fo.at[0], s_out).wait()

    @pl.when(c != zh)
    def _():
        pltpu.make_async_copy(fo.at[0], fo.at[0], s_next).wait()

    to_pair.wait_send()
    sent = p1.at[pl.ds(0, 31), pl.ds(0, PIECE)]
    pltpu.make_async_copy(sent, sent, s_p1).wait()
    pltpu.make_async_copy(sent, sent, s_p2).wait()

    @pl.when(zl == 0)
    def _():
        last = p1.at[pl.ds(0, 31), PIECE]
        pltpu.make_async_copy(last, last, s_last).wait()
        more = p1.at[pl.ds(0, 7), PIECE]
        pltpu.make_async_copy(more, more, s_more).wait()

    @pl.when(zl != 0)
    def _():
        more = p1.at[pl.ds(0, 8), PIECE]
        pltpu.make_async_copy(more, more, s_more).wait()

    for copy in bias_sends + do + [dq, d1, d2]:
        copy.wait_send()
    for ring in (zq, zo, z1, z2, xq, xo, x1, x2, yo):
        ring.drain()

    @pl.loop(0, CHUNKS)
    def _(t):
        yx(t).drain()
        dkv(t).wait_send()
        yn(t).drain()
        for i in range(1, 4):
            context_send(t, i).wait_send()
        for copy in sums(t):
            copy.wait_send()


def on_device(
    frames_in, ln1_gain, ln1_bias, qkv_weight, qv_bias, out_weight, out_bias,
    ln2_gain, ln2_bias, fc1_weight, fc1_bias, fc2_weight, fc2_bias, server_of_clip,
):
    smem = pl.BlockSpec(memory_space=pltpu.SMEM)
    dma = pltpu.SemaphoreType.DMA
    V = pltpu.VMEM
    out = pl.pallas_call(
        kernel,
        out_shape=jax.ShapeDtypeStruct((320, 640), BF16),
        in_specs=[smem] + [pl.BlockSpec(memory_space=pl.ANY)] * 13,
        out_specs=pl.BlockSpec(memory_space=pl.ANY),
        scratch_shapes=[
            pltpu.SMEM((32,), jnp.int32), pltpu.SMEM((32,), jnp.int32), pltpu.SMEM((32,), jnp.int32),
            V((320, 640), BF16), V((3, 40, 128), BF16), V((4, D), BF16), V((20, D), BF16),
            V((2, 128), F32), V((1, 160), F32), V((5, 128), F32), V((1, 160), F32),
            V((10, 128), F32), V((10, 128), F32), V((10, 128), F32), V((10, 128), F32),
            V((4, D), F32),
            V((2, TILES, 8, 128), BF16),
            V((32, PIECE + 1, 8, 128), BF16),
            V((32, PIECE + 1, 8, 128), BF16),
            V((4, 2, TILES, 8, 128), BF16),
            V((2, 4, 4, 2, 40, 384), BF16),
            V((2, 4, 4, 2, 40, 640), BF16),
            V((2, 2, 4, 4, 40, 640), BF16),
            V((2, 4, 2, 4, 4, 8, 640), BF16),
            V((2, 24, 640), BF16),
            V((2, 24, 640), BF16),
            V((8, 640), F32),
            V((8, 8, 640), F32),
            V((4, HALF, D), BF16),
            V((4, ROWS, D), BF16),
            V((CHUNKS, 4 * ROWS, 256), BF16),
            V((2, CHUNKS, 2, 4 * ROWS, 256), BF16),
            V((CHUNKS, 4, ROWS, 256), BF16),
            V((4, HALF, 256), BF16),
            V((HALF, D), F32),
            V((4, HALF, D), BF16),
            V((4, 2, HALF, 640), BF16),
            V((HALF, 640), BF16),
            V((HALF, 640), BF16),
            V((2, HALF, 640), BF16),
            V((2, HALF, 640), BF16),
            V((2, HALF, 640), BF16),
            dma((13,)), dma((3,)),
            dma, dma, dma, dma, dma, dma, dma, dma, dma, dma((8,)), dma((8,)),
            dma((7,)), dma((7,)), dma((7,)), dma((7,)), dma((7,)), dma((7,)), dma((7,)), dma((7,)),
            dma((4,)), dma((4,)), dma((4,)), dma((4,)), dma((4,)), dma((4,)), dma((4,)), dma((4,)),
            dma((4 * CHUNKS,)), dma((4 * CHUNKS,)), dma((4,)), dma((4,)),
            dma((4 * CHUNKS,)), dma((4 * CHUNKS,)),
            dma((8,)), dma((8,)), dma((CHUNKS,)), dma((CHUNKS,)), dma((3 * CHUNKS,)), dma((3 * CHUNKS,)), dma((4 * CHUNKS,)), dma((4 * CHUNKS,)),
            dma, dma, dma,
        ],
        compiler_params=pltpu.CompilerParams(
            collective_id=0, has_side_effects=True, vmem_limit_bytes=60 * 2**20
        ),
    )(
        server_of_clip, frames_in.reshape(320, 640), qkv_weight.transpose(1, 0, 2), fc1_weight,
        out_weight, fc2_weight, qv_bias, out_bias[None], fc1_bias.reshape(5, 128), fc2_bias[None],
        ln1_gain.reshape(10, 128), ln1_bias.reshape(10, 128),
        ln2_gain.reshape(10, 128), ln2_bias.reshape(10, 128),
    )
    return out.reshape(1, 1, 320, 640)


def solution(mesh):
    torus = Mesh(mesh.devices.reshape(4, 4, 2, 4, 2), ("x", "zl", "c", "y", "zh"))
    return jax.shard_map(
        on_device,
        mesh=torus,
        in_specs=(
            P(DP, HEAD, None, None), P(), P(), P(DP, None, HEAD), P(None, HEAD), P(HEAD_DP, None),
            P(HEAD), P(), P(), P(DP, HEAD), P(HEAD), P(HEAD_DP, None), P(HEAD), P(),
        ),
        out_specs=P(DP, HEAD, None, None),
        check_vma=False,
    )
```

```python
import functools

import jax
import jax.numpy as jnp
from jax import lax
from jax.experimental import pallas as pl
from jax.experimental.pallas import tpu as pltpu
from jax.sharding import Mesh
from jax.sharding import PartitionSpec as P

MESH = pl.DeviceIdType.MESH
BF16 = jnp.bfloat16
F32 = jnp.float32
EPS = 1e-05
HDIM = 64
DP = ("x", "zl", "c")
HEAD = ("y", "zh")
HEAD_DP = ("y", "zh", "x", "zl", "c")

D = 1280
HALF = 160
TILES = 100
PART = 3
FIRST = 16 * PART
CHUNKS = 5
ROWS = 32


def remote(src, dst, send, recv, device):
    return pltpu.make_async_remote_copy(
        src_ref=src, dst_ref=dst, send_sem=send, recv_sem=recv,
        device_id=device, device_id_type=MESH,
    )


class Ring4:
    def __init__(self, slab, half, i, device, send, recv, base=0):
        up, down = lax.rem(i + 1, 4), lax.rem(i + 3, 4)
        own = slab(i)

        def sems(n):
            return send.at[base + n], recv.at[base + n]

        self.one = [
            remote(own, own, *sems(0), device(up)),
            remote(own, own, *sems(1), device(down)),
        ]
        self.two = [
            remote(half(down, 0), half(down, 0), *sems(2), device(up)),
            remote(half(up, 1), half(up, 1), *sems(3), device(down)),
        ]

    def start(self):
        for copy in self.one:
            copy.start()

    def forward(self):
        for copy, nxt in zip(self.one, self.two):
            copy.wait_recv()
            nxt.start()

    def arrive(self):
        for copy in self.two:
            copy.wait_recv()

    def drain(self):
        for copy in self.one + self.two:
            copy.wait_send()


class Ring8:
    def __init__(self, slab, i, device, send, recv):
        up, down = lax.rem(i + 1, 8), lax.rem(i + 7, 8)
        self.steps = []
        for s in range(4):
            older = slab(lax.rem(i + 8 - s, 8))
            copies = [remote(older, older, send.at[2 * s], recv.at[2 * s], device(up))]
            if s < 3:
                newer = slab(lax.rem(i + s, 8))
                copies.append(
                    remote(newer, newer, send.at[2 * s + 1], recv.at[2 * s + 1], device(down))
                )
            self.steps.append(copies)

    def start(self, s):
        for copy in self.steps[s]:
            copy.start()

    def arrive(self, s):
        for copy in self.steps[s]:
            copy.wait_recv()

    def relay(self, s):
        self.arrive(s)
        if s < 3:
            self.start(s + 1)

    def drain(self):
        for copies in self.steps:
            for copy in copies:
                copy.wait_send()


class Two8:
    def __init__(self, slab, i, device, send, recv):
        def to(block, step, n):
            return remote(
                block, block, send.at[n], recv.at[n], device(lax.rem(i + 8 + step, 8))
            )

        own, low, high = slab(i), slab(lax.rem(i + 6, 8)), slab(lax.rem(i + 2, 8))
        self.one = [to(own, step, n) for n, step in enumerate((1, -1, 2, -2))]
        self.two = [to(low, 1, 4), to(high, -1, 5), to(low, 2, 6)]

    def start(self):
        for copy in self.one:
            copy.start()

    def forward(self):
        for copy in self.one:
            copy.wait_recv()
        for copy in self.two:
            copy.start()

    def arrive(self):
        for copy in self.two:
            copy.wait_recv()

    def drain(self):
        for copy in self.one + self.two:
            copy.wait_send()


def layer_norm(floats, gain, shift):
    center = jnp.sum(floats, axis=-1, keepdims=True) * (1.0 / D)
    moved = floats - center
    spread = jnp.sum(moved * moved, axis=-1, keepdims=True) * (1.0 / D)
    return (moved * lax.rsqrt(spread + EPS) * gain + shift).astype(BF16)


def dot(a, b):
    return jnp.dot(a, b, preferred_element_type=F32)


def kernel(
    servers, frames_hbm, qkv_hbm, fc1_in, out_hbm, fc2_hbm, qv_hbm, bo_hbm, b1_hbm, b2_hbm,
    g1_hbm, s1_hbm, g2_hbm, s2_hbm,
    out,
    keys, slots, order, frames, qkv_in, out_in, fc2_in, b_qv, b_out, b_fc1, b_fc2, g1, s1, g2, s2,
    norms, fin, p1, pb, pm, p2, xg, wq, w1, w2, wo, tail, pair, bias, bg, xr, xn, qs, kv, cs, cx, att, n2, pk,
    ra, rb, rc, rd, fo,
    fetch, local, s_p1, r_p1, s_p2, r_p2, r_b1, r_b2, s_more, r_more, s_last, s_pair, r_pair, s_bias, r_bias,
    s_zq, r_zq, s_zo, r_zo, s_z1, r_z1, s_z2, r_z2,
    s_xq, r_xq, s_xo, r_xo, s_x1, r_x1, s_x2, r_x2,
    s_yx, r_yx, s_yo, r_yo, s_yn, r_yn, s_d, r_d, s_kv, r_kv, s_cx, r_cx, s_rs, r_rs, s_out, s_next, r_out,
):
    x, zl, c = lax.axis_index("x"), lax.axis_index("zl"), lax.axis_index("c")
    y, zh = lax.axis_index("y"), lax.axis_index("zh")
    z = zh * 4 + zl
    clip = x * 8 + zl * 2 + c

    def at(x_=x, zl_=zl, c_=c, y_=y, zh_=zh):
        return (x_, zl_, c_, y_, zh_)

    def at_z(z_):
        return at(zl_=lax.rem(z_, 4), zh_=z_ // 4)

    def at_x(i):
        return at(x_=i)

    def at_y(i):
        return at(y_=i)

    sibling = at(c_=1 - c)

    fetches = [
        pltpu.make_async_copy(src, dst, fetch.at[n])
        for n, (src, dst) in enumerate(
            [(frames_hbm, frames), (out_hbm, out_in), (fc2_hbm, fc2_in), (qkv_hbm, qkv_in),
             (qv_hbm, b_qv), (bo_hbm, b_out), (b1_hbm, b_fc1), (b2_hbm, b_fc2), (g1_hbm, g1),
             (s1_hbm, s1), (g2_hbm, g2), (s2_hbm, s2), (fc1_in, w1.at[zh, x, zl, c])]
        )
    ]
    for copy in fetches:
        copy.start()
    barrier = pltpu.get_barrier_semaphore()

    def greet(device):
        pl.semaphore_signal(barrier, inc=1, device_id=device, device_id_type=MESH)

    @pl.loop(0, 16)
    def _(i):
        t = lax.rem(x * 4 + zl + i, 16)
        greet(at(x_=t // 4, zl_=lax.rem(t, 4), zh_=1 - zh))

    @pl.loop(1, 32)
    def _(i):
        t = lax.rem(clip + i, 32)
        greet(at(x_=t // 8, zl_=lax.rem(t // 2, 4), c_=lax.rem(t, 2)))

    greet(at(c_=1 - c, zh_=1 - zh))
    for i in range(1, 4):
        greet(at(y_=lax.rem(y + i, 4)))
        greet(at(y_=lax.rem(y + i, 4), zh_=1 - zh))

    for copy in fetches:
        copy.wait()

    for half in range(2):
        for tile in range(100):
            rt, lt = half * 20 + tile // 5, tile % 5
            fin[half, tile] = frames[8 * rt : 8 * rt + 8, 128 * lt : 128 * lt + 128]
    for h in range(2):
        tail[h, 0:4] = out_in[:, 640 * h : 640 * h + 640]
        tail[h, 4:24] = fc2_in[:, 640 * h : 640 * h + 640]
    for t in range(3):
        wq[zh, x, zl, c, :, 128 * t : 128 * t + 128] = qkv_in[t]
    def flat(ref):
        return jnp.concatenate([ref[i : i + 1] for i in range(ref.shape[0])], axis=1)

    bias[0:1, :] = flat(b_fc1)
    for i, ref in enumerate((g1, s1, g2, s2)):
        norms[i : i + 1] = flat(ref)
    bias[1:2, 0:160] = b_out[...]
    bias[2:3, 0:160] = b_fc2[...]
    bias[3:5, 0:128] = b_qv[...]

    zq = Two8(lambda i: wq.at[i // 4, x, lax.rem(i, 4), c], z, at_z, s_zq, r_zq)
    zo = Two8(lambda i: wo.at[c, y, i // 4, x, lax.rem(i, 4)], z, at_z, s_zo, r_zo)
    z1 = Two8(lambda i: w1.at[i // 4, x, lax.rem(i, 4), c], z, at_z, s_z1, r_z1)
    z2 = Ring8(lambda i: w2.at[c, i // 4, :, lax.rem(i, 4)], z, at_z, s_z2, r_z2)
    xq = Ring4(lambda i: wq.at[:, i, :, c], lambda i, h: wq.at[h, i, :, c], x, at_x, s_xq, r_xq)
    xo = Ring4(lambda i: wo.at[c, y, :, i], lambda i, h: wo.at[c, y, h, i], x, at_x, s_xo, r_xo)
    x1 = Ring4(lambda i: w1.at[:, i, :, c], lambda i, h: w1.at[h, i, :, c], x, at_x, s_x1, r_x1)
    x2 = Ring4(
        lambda i: w2.at[c, zh, i, zl],
        lambda i, h: w2.at[c, zh, i, zl, pl.ds(24 * h, 24 - 8 * h)],
        x, at_x, s_x2, r_x2,
    )
    yo = Ring4(lambda i: wo.at[c, i], lambda i, h: wo.at[c, i, h], y, at_y, s_yo, r_yo)

    def yx(t):
        tiles = pl.ds(t * 20, 20)
        return Ring4(
            lambda i: xg.at[i, :, tiles], lambda i, h: xg.at[i, h, tiles], y, at_y, s_yx, r_yx, t * 4
        )

    def yn(t):
        def rows(first, count):
            return pl.ds(pl.multiple_of(t * ROWS + first, 16), count)

        return Ring4(
            lambda i: n2.at[i, rows(0, ROWS)], lambda i, h: n2.at[i, rows(16 * h, 16)],
            y, at_y, s_yn, r_yn, t * 4,
        )

    dq = remote(wq.at[:, :, :, c], wq.at[:, :, :, c], s_d.at[0], r_d.at[0], sibling)
    d1 = remote(w1.at[:, :, :, c], w1.at[:, :, :, c], s_d.at[1], r_d.at[1], sibling)
    d2 = remote(w2.at[c], w2.at[c], s_d.at[2], r_d.at[2], sibling)

    def dkv(t):
        return remote(kv.at[c, t], kv.at[c, t], s_kv.at[t], r_kv.at[t], sibling)

    do = []
    for n in range(4):
        part = wo.at[c, lax.rem(y + (0, 1, 3, 2)[n], 4)]
        do.append(remote(part, part, s_d.at[3 + n], r_d.at[3 + n], sibling))
    bias_sends = []
    for i in range(4):
        for other in range(2):
            if i or other:
                device = at(y_=lax.rem(y + i, 4), zh_=(1 - zh) if other else zh)
                n = i * 2 + other
                bias_sends.append(
                    remote(bias, bg.at[y * 2 + zh], s_bias.at[n], r_bias.at[n], device)
                )
    own_b = pltpu.make_async_copy(bias, bg.at[y * 2 + zh], local.at[1])
    own_pair = pltpu.make_async_copy(tail.at[c], pair.at[c], local.at[2])
    to_pair = remote(tail.at[1 - c], pair.at[c], s_pair, r_pair, sibling)

    pl.semaphore_wait(barrier, 54)

    to_pair.start()
    zq.start()
    own_b.start()
    own_pair.start()

    def tiles_of(x_, zl_, second):
        if second:
            return FIRST + x_ * 13 + zl_ * PART + jnp.minimum(zl_, 1)
        return (x_ * 4 + zl_) * PART

    def regroup_sends(first, last, second):
        landing, arrived_at = (p1, pb)[second], (r_p1, r_b1)[second]

        @pl.loop(first, last)
        def _(i):
            t = lax.rem(clip + i, 32)
            x_, zl_, c_ = t // 8, lax.rem(t // 2, 4), lax.rem(t, 2)
            tile = tiles_of(x_, zl_, second)
            device = at(x_=x_, zl_=zl_, c_=c_)
            remote(
                fin.at[c_, pl.ds(tile, PART)], landing.at[clip], s_p1, arrived_at, device
            ).start()
            if second:
                @pl.when(zl_ == 0)
                def _():
                    remote(
                        fin.at[c_, tile + PART], pm.at[clip], s_more, r_more, device
                    ).start()

    own_tiles = [tiles_of(x, zl, second) for second in range(2)]
    own_more = own_tiles[1] + PART
    for second in range(2):
        pltpu.make_async_copy(
            fin.at[c, pl.ds(own_tiles[second], PART)],
            (p1, pb)[second].at[clip],
            (r_p1, r_b1)[second],
        ).start()

    @pl.when(zl == 0)
    def _():
        pltpu.make_async_copy(fin.at[c, own_more], pm.at[clip], r_more).start()

    regroup_sends(1, 32, 0)
    own_pair.wait()
    to_pair.wait_recv()
    wo[c, y, zh, x, zl, 0:4] = pair[0, 0:4]
    wo[c, y, zh, x, zl, 4:8] = pair[1, 0:4]
    w2[c, zh, x, zl, 0:20] = pair[0, 4:24]
    w2[c, zh, x, zl, 20:40] = pair[1, 4:24]
    x2.start()

    for i in range(32):
        keys[i] = servers[i] * 32 + i

    @pl.loop(0, 32)
    def _(i):
        own, total = keys[i], jnp.int32(0)
        for other in range(32):
            total = total + jnp.where(keys[other] < own, 1, 0)
        slots[i] = total

    zq.forward()
    regroup_sends(1, 32, 1)

    @pl.loop(0, 32)
    def _(i):
        total = jnp.int32(0)
        for other in range(32):
            total = total + jnp.where(slots[other] == i, other, 0)
        order[i] = total

    own_b.wait()

    slot = x * 8 + zl * 2 + zh

    def slot_sends(second):
        part, arrived_at = pl.ds(PART * second, PART), (r_p2, r_b2)[second]
        landing = (p1, pb)[second]
        pltpu.make_async_copy(landing, landing, (r_p1, r_b1)[second]).wait()

        @pl.loop(0, 32)
        def _(s):
            p2[s, part] = landing[order[s]]

        place = xg.at[y, zh, pl.ds(own_tiles[second], PART)]
        place_more = xg.at[y, zh, own_more]
        if second:
            @pl.when(zl == 0)
            def _():
                pltpu.make_async_copy(pm, pm, r_more).wait()

                @pl.loop(0, 32)
                def _(s):
                    p2[s, 2 * PART] = pm[order[s]]

        @pl.loop(1, 32)
        def _(i):
            t = lax.rem(slot + i, 32)
            device = at(x_=t // 8, zl_=lax.rem(t // 2, 4), zh_=lax.rem(t, 2))
            remote(p2.at[t, part], place, s_p2, arrived_at, device).start()
            if second:
                @pl.when(zl == 0)
                def _():
                    remote(p2.at[t, 2 * PART], place_more, s_last, arrived_at, device).start()

        pltpu.make_async_copy(p2.at[slot, part], place, arrived_at).start()
        if second:
            @pl.when(zl == 0)
            def _():
                pltpu.make_async_copy(p2.at[slot, 2 * PART], place_more, arrived_at).start()

    slot_sends(0)
    zo.start()
    zq.arrive()
    xq.start()
    slot_sends(1)
    x2.forward()
    for copy in bias_sends:
        copy.start()
    here = xg.at[y, :, pl.ds(0, FIRST)]
    pltpu.make_async_copy(here, here, r_p2).wait()
    yx(0).start()
    yx(1).start()
    zo.forward()
    z1.start()
    xq.forward()
    yx(0).forward()
    x2.arrive()
    here = xg.at[y, :, pl.ds(FIRST, TILES - FIRST)]
    pltpu.make_async_copy(here, here, r_b2).wait()
    yx(2).start()
    yx(1).forward()
    yx(3).start()
    xq.arrive()
    dq.start()
    for copy in bias_sends:
        copy.wait_recv()
    dq.wait_recv()
    zo.arrive()
    xo.start()

    def project(t):
        @pl.loop(0, 2)
        def _(u):
            first = t * 20 + u * 10
            blocks = []
            for b in range(8):
                parts = [
                    jnp.concatenate(
                        [xg[b // 2, b % 2, first + lt], xg[b // 2, b % 2, first + 5 + lt]], axis=0
                    )
                    for lt in range(5)
                ]
                blocks.append(jnp.concatenate(parts, axis=1))
            start = pl.multiple_of(t * ROWS + u * 16, 16)
            inner = pl.multiple_of(u * 16, 16)
            for j in range(4):
                whole = jnp.concatenate(
                    [block[:, 160 * j : 160 * j + 160] for block in blocks], axis=1
                )
                xr[j, pl.ds(start, 16)] = whole
                xn[j, pl.ds(inner, 16)] = layer_norm(whole.astype(F32), norms[0:1], norms[1:2])

        left = xn[...].reshape(4 * ROWS, D)
        for h in range(2):
            prod = dot(left, wq[h].reshape(D, 384))
            biases = bg[y * 2 + h]
            lanes = slice(128 * h, 128 * h + 128)
            query = ((prod[:, 0:128] + biases[3:4, 0:128]) * HDIM ** (-0.5)).astype(BF16)
            key = prod[:, 128:256].astype(BF16)
            value = (prod[:, 256:384] + biases[4:5, 0:128]).astype(BF16)
            qs[t, :, lanes] = query
            kv[c, t, 0, :, lanes] = key
            kv[c, t, 1, :, lanes] = value
        dkv(t).start()

    @pl.loop(0, CHUNKS)
    def _(t):
        with jax.named_scope("L_fwd"):
            @pl.when(t < CHUNKS - 2)
            def _():
                yx(t + 2).forward()

            @pl.when(t < CHUNKS - 4)
            def _():
                yx(t + 4).start()

        with jax.named_scope("L_z1"):
            @pl.when(t == 0)
            def _():
                z1.forward()
                z2.start(0)

            @pl.when(t == 1)
            def _():
                xo.forward()

            @pl.when(t == 2)
            def _():
                z1.arrive()
                x1.start()

            @pl.when(t == 3)
            def _():
                xo.arrive()
                yo.start()
                do[0].start()

        with jax.named_scope("L_arr"):
            yx(t).arrive()
        with jax.named_scope("L_proj"):
            project(t)

    z2.relay(0)
    for t in range(CHUNKS):
        dkv(t).wait_recv()

    head_of = lax.broadcasted_iota(jnp.int32, (4 * ROWS, 256), 1) // HDIM

    def rows_of(t):
        return pl.ds(pl.multiple_of(t * ROWS, ROWS), ROWS)

    def context_send(t, i):
        j = lax.rem(y + i, 4)
        n = 3 * t + i - 1
        return remote(cs.at[t, j], cx.at[y, rows_of(t)], s_cx.at[n], r_cx.at[n], at(y_=j))

    def attend(t):
        q = qs[t]
        zero = jnp.zeros_like(q)
        stacked = jnp.concatenate([jnp.where(head_of == h, q, zero) for h in range(4)], axis=0)
        keys = kv[:, :, 0].reshape(D, 256)
        scores = lax.dot_general(
            stacked, keys, (((1,), (1,)), ((), ())), preferred_element_type=F32
        )
        weights = jnp.exp(scores - jnp.max(scores, axis=-1, keepdims=True))
        total = jnp.sum(weights, axis=-1, keepdims=True)
        mixed = dot(weights.astype(BF16), kv[:, :, 1].reshape(D, 256)) / total
        context = jnp.zeros((4 * ROWS, 256), F32)
        for h in range(4):
            part = mixed[h * 4 * ROWS : (h + 1) * 4 * ROWS]
            context = context + jnp.where(head_of == h, part, 0.0)
        context = context.astype(BF16)
        for j in range(4):
            cs[t, j] = context[j * ROWS : (j + 1) * ROWS]
        for i in (2, 1, 3):
            context_send(t, i).start()
        cx[y, rows_of(t)] = cs[t, y]

    def whole_bias(row):
        return jnp.concatenate([bg[h, row : row + 1, 0:160] for h in range(8)], axis=1)

    def attend_out(t):
        r = rows_of(t)
        for i in range(1, 4):
            context_send(t, i).wait_recv()
        context = jnp.concatenate([cx[i, r] for i in range(4)], axis=1)
        product = jnp.concatenate(
            [dot(context, wo[h].reshape(1024, 640)) for h in range(2)], axis=1
        )
        attended = (xr[y, r].astype(F32) + whole_bias(1) + product).astype(BF16)
        att[r] = attended.astype(F32) + whole_bias(2)
        n2[y, r] = layer_norm(attended.astype(F32), norms[2:3], norms[3:4])
        yn(t).start()

    up, down, far = lax.rem(y + 1, 4), lax.rem(y + 3, 4), lax.rem(y + 2, 4)

    def sums(t):
        r, n = rows_of(t), 4 * t
        return [
            remote(pk.at[far, 0, r], ra.at[r], s_rs.at[n], r_rs.at[n], at(y_=up)),
            remote(pk.at[far, 1, r], rb.at[r], s_rs.at[n + 1], r_rs.at[n + 1], at(y_=down)),
            remote(pk.at[up, :, r], rc.at[:, r], s_rs.at[n + 2], r_rs.at[n + 2], at(y_=up)),
            remote(pk.at[down, :, r], rd.at[:, r], s_rs.at[n + 3], r_rs.at[n + 3], at(y_=down)),
        ]

    def feed_forward(t):
        r = rows_of(t)
        left = jnp.concatenate([n2[j, r] for j in range(4)], axis=0)
        parts = []
        for h in range(2):
            total = dot(left, w1[h].reshape(D, 640)) + bg[y * 2 + h, 0:1, :]
            parts.append((0.5 * total * (1.0 + lax.erf(total * 0.5**0.5))).astype(BF16))
        hidden = jnp.concatenate(parts, axis=1)

        @pl.when(t == 0)
        def _():
            d2.wait_recv()

        share = jnp.concatenate(
            [dot(hidden, w2[h].reshape(D, 640)) for h in range(2)], axis=1
        )
        kept = att[r]
        for j in range(4):
            part = share[ROWS * j : ROWS * j + ROWS] + jnp.where(y == j, kept, 0.0)
            for b in range(8):
                pk[b // 2, b % 2, r, 160 * j : 160 * j + 160] = part[
                    :, 160 * b : 160 * b + 160
                ].astype(BF16)
        sums(t)[0].start()
        sums(t)[1].start()

    def add_and_pass(t):
        r = rows_of(t)
        copies = sums(t)
        copies[0].wait_recv()
        pk[up, 0, r] = (pk[up, 0, r].astype(F32) + ra[r].astype(F32)).astype(BF16)
        copies[2].start()
        copies[1].wait_recv()
        pk[down, 1, r] = (pk[down, 1, r].astype(F32) + rb[r].astype(F32)).astype(BF16)
        copies[3].start()

    def out_rows(t):
        return out.at[pl.ds(pl.multiple_of(c * HALF + t * ROWS, ROWS), ROWS)]

    def finish(t):
        r = rows_of(t)
        copies = sums(t)
        copies[2].wait_recv()
        copies[3].wait_recv()
        fo[:, r] = (pk[y, :, r].astype(F32) + rc[:, r].astype(F32) + rd[:, r].astype(F32)).astype(
            BF16
        )
        remote(fo.at[1 - zh, r], out_rows(t), s_out, r_out, at(c_=zh, zh_=1 - zh)).start()

        @pl.when(c == zh)
        def _():
            pltpu.make_async_copy(fo.at[zh, r], out_rows(t), r_out).start()

        @pl.when(c != zh)
        def _():
            remote(fo.at[zh, r], out_rows(t), s_next, r_out, sibling).start()

    @pl.loop(0, CHUNKS)
    def _(t):
        with jax.named_scope("M_att"):
            attend(t)

        with jax.named_scope("M_w"):
            @pl.when(t == 1)
            def _():
                yo.forward()
                do[1].start()
                do[2].start()

            @pl.when(t == 2)
            def _():
                x1.forward()
                z2.relay(1)

    yo.arrive()
    do[3].start()
    for copy in do:
        copy.wait_recv()

    @pl.loop(0, CHUNKS)
    def _(t):
        with jax.named_scope("O_out"):
            attend_out(t)

        with jax.named_scope("O_z2"):
            @pl.when(t == 0)
            def _():
                z2.relay(2)
                x1.arrive()
                d1.start()

            @pl.when(t == CHUNKS - 1)
            def _():
                z2.arrive(3)
                d2.start()

        with jax.named_scope("O_fwd"):
            @pl.when(t > 1)
            def _():
                yn(t - 2).forward()

    d1.wait_recv()

    @pl.loop(0, CHUNKS + 2)
    def _(i):
        @pl.when(i < CHUNKS)
        def _():
            with jax.named_scope("M_arr"):
                yn(i).arrive()
            with jax.named_scope("M_ff"):
                feed_forward(i)
            with jax.named_scope("M_fwd"):
                @pl.when(i < 2)
                def _():
                    yn(i + 3).forward()

        with jax.named_scope("M_add"):
            @pl.when((i > 0) & (i <= CHUNKS))
            def _():
                add_and_pass(i - 1)

        with jax.named_scope("M_fin"):
            @pl.when(i > 1)
            def _():
                finish(i - 2)

    pltpu.make_async_copy(out, out, r_out).wait()

    pltpu.make_async_copy(fo.at[0], fo.at[0], s_out).wait()

    @pl.when(c != zh)
    def _():
        pltpu.make_async_copy(fo.at[0], fo.at[0], s_next).wait()

    to_pair.wait_send()
    sent = p2.at[pl.ds(0, 31), pl.ds(0, 2 * PART)]
    pltpu.make_async_copy(sent, sent, s_p1).wait()
    pltpu.make_async_copy(sent, sent, s_p2).wait()

    @pl.when(zl == 0)
    def _():
        last = p2.at[pl.ds(0, 31), 2 * PART]
        pltpu.make_async_copy(last, last, s_last).wait()
        more = pm.at[pl.ds(0, 7)]
        pltpu.make_async_copy(more, more, s_more).wait()

    @pl.when(zl != 0)
    def _():
        more = pm.at[pl.ds(0, 8)]
        pltpu.make_async_copy(more, more, s_more).wait()

    for copy in bias_sends + do + [dq, d1, d2]:
        copy.wait_send()
    for ring in (zq, zo, z1, z2, xq, xo, x1, x2, yo):
        ring.drain()

    @pl.loop(0, CHUNKS)
    def _(t):
        yx(t).drain()
        dkv(t).wait_send()
        yn(t).drain()
        for i in range(1, 4):
            context_send(t, i).wait_send()
        for copy in sums(t):
            copy.wait_send()


def on_device(
    frames_in, ln1_gain, ln1_bias, qkv_weight, qv_bias, out_weight, out_bias,
    ln2_gain, ln2_bias, fc1_weight, fc1_bias, fc2_weight, fc2_bias, server_of_clip,
):
    smem = pl.BlockSpec(memory_space=pltpu.SMEM)
    dma = pltpu.SemaphoreType.DMA
    V = pltpu.VMEM
    out = pl.pallas_call(
        kernel,
        out_shape=jax.ShapeDtypeStruct((320, 640), BF16),
        in_specs=[smem] + [pl.BlockSpec(memory_space=pl.ANY)] * 13,
        out_specs=pl.BlockSpec(memory_space=pl.ANY),
        scratch_shapes=[
            pltpu.SMEM((32,), jnp.int32), pltpu.SMEM((32,), jnp.int32), pltpu.SMEM((32,), jnp.int32),
            V((320, 640), BF16), V((3, 40, 128), BF16), V((4, D), BF16), V((20, D), BF16),
            V((2, 128), F32), V((1, 160), F32), V((5, 128), F32), V((1, 160), F32),
            V((10, 128), F32), V((10, 128), F32), V((10, 128), F32), V((10, 128), F32),
            V((4, D), F32),
            V((2, TILES, 8, 128), BF16),
            V((32, PART, 8, 128), BF16),
            V((32, PART, 8, 128), BF16),
            V((32, 8, 128), BF16),
            V((32, 2 * PART + 1, 8, 128), BF16),
            V((4, 2, TILES, 8, 128), BF16),
            V((2, 4, 4, 2, 40, 384), BF16),
            V((2, 4, 4, 2, 40, 640), BF16),
            V((2, 2, 4, 4, 40, 640), BF16),
            V((2, 4, 2, 4, 4, 8, 640), BF16),
            V((2, 24, 640), BF16),
            V((2, 24, 640), BF16),
            V((8, 640), F32),
            V((8, 8, 640), F32),
            V((4, HALF, D), BF16),
            V((4, ROWS, D), BF16),
            V((CHUNKS, 4 * ROWS, 256), BF16),
            V((2, CHUNKS, 2, 4 * ROWS, 256), BF16),
            V((CHUNKS, 4, ROWS, 256), BF16),
            V((4, HALF, 256), BF16),
            V((HALF, D), F32),
            V((4, HALF, D), BF16),
            V((4, 2, HALF, 640), BF16),
            V((HALF, 640), BF16),
            V((HALF, 640), BF16),
            V((2, HALF, 640), BF16),
            V((2, HALF, 640), BF16),
            V((2, HALF, 640), BF16),
            dma((13,)), dma((3,)),
            dma, dma, dma, dma, dma, dma, dma, dma, dma, dma, dma, dma((8,)), dma((8,)),
            dma((7,)), dma((7,)), dma((7,)), dma((7,)), dma((7,)), dma((7,)), dma((7,)), dma((7,)),
            dma((4,)), dma((4,)), dma((4,)), dma((4,)), dma((4,)), dma((4,)), dma((4,)), dma((4,)),
            dma((4 * CHUNKS,)), dma((4 * CHUNKS,)), dma((4,)), dma((4,)),
            dma((4 * CHUNKS,)), dma((4 * CHUNKS,)),
            dma((8,)), dma((8,)), dma((CHUNKS,)), dma((CHUNKS,)), dma((3 * CHUNKS,)), dma((3 * CHUNKS,)), dma((4 * CHUNKS,)), dma((4 * CHUNKS,)),
            dma, dma, dma,
        ],
        compiler_params=pltpu.CompilerParams(
            collective_id=0, has_side_effects=True, vmem_limit_bytes=60 * 2**20
        ),
    )(
        server_of_clip, frames_in.reshape(320, 640), qkv_weight.transpose(1, 0, 2), fc1_weight,
        out_weight, fc2_weight, qv_bias, out_bias[None], fc1_bias.reshape(5, 128), fc2_bias[None],
        ln1_gain.reshape(10, 128), ln1_bias.reshape(10, 128),
        ln2_gain.reshape(10, 128), ln2_bias.reshape(10, 128),
    )
    return out.reshape(1, 1, 320, 640)


def solution(mesh):
    torus = Mesh(mesh.devices.reshape(4, 4, 2, 4, 2), ("x", "zl", "c", "y", "zh"))
    return jax.shard_map(
        on_device,
        mesh=torus,
        in_specs=(
            P(DP, HEAD, None, None), P(), P(), P(DP, None, HEAD), P(None, HEAD), P(HEAD_DP, None),
            P(HEAD), P(), P(), P(DP, HEAD), P(HEAD), P(HEAD_DP, None), P(HEAD), P(),
        ),
        out_specs=P(DP, HEAD, None, None),
        check_vma=False,
    )
```

```python
import functools

import jax
import jax.numpy as jnp
from jax import lax
from jax.experimental import pallas as pl
from jax.experimental.pallas import tpu as pltpu
from jax.sharding import Mesh
from jax.sharding import PartitionSpec as P

MESH = pl.DeviceIdType.MESH
BF16 = jnp.bfloat16
F32 = jnp.float32
EPS = 1e-05
HDIM = 64
DP = ("x", "zl", "c")
HEAD = ("y", "zh")
HEAD_DP = ("y", "zh", "x", "zl", "c")

D = 1280
HALF = 160
TILES = 100
PART = 3
FIRST = 16 * PART
CHUNKS = 5
ROWS = 32


def remote(src, dst, send, recv, device):
    return pltpu.make_async_remote_copy(
        src_ref=src, dst_ref=dst, send_sem=send, recv_sem=recv,
        device_id=device, device_id_type=MESH,
    )


class Ring4:
    def __init__(self, slab, half, i, device, send, recv, base=0):
        up, down = lax.rem(i + 1, 4), lax.rem(i + 3, 4)
        own = slab(i)

        def sems(n):
            return send.at[base + n], recv.at[base + n]

        self.one = [
            remote(own, own, *sems(0), device(up)),
            remote(own, own, *sems(1), device(down)),
        ]
        self.two = [
            remote(half(down, 0), half(down, 0), *sems(2), device(up)),
            remote(half(up, 1), half(up, 1), *sems(3), device(down)),
        ]

    def start(self):
        for copy in self.one:
            copy.start()

    def forward(self):
        for copy, nxt in zip(self.one, self.two):
            copy.wait_recv()
            nxt.start()

    def arrive(self):
        for copy in self.two:
            copy.wait_recv()

    def drain(self):
        for copy in self.one + self.two:
            copy.wait_send()


class Ring8:
    def __init__(self, slab, i, device, send, recv):
        up, down = lax.rem(i + 1, 8), lax.rem(i + 7, 8)
        self.steps = []
        for s in range(4):
            older = slab(lax.rem(i + 8 - s, 8))
            copies = [remote(older, older, send.at[2 * s], recv.at[2 * s], device(up))]
            if s < 3:
                newer = slab(lax.rem(i + s, 8))
                copies.append(
                    remote(newer, newer, send.at[2 * s + 1], recv.at[2 * s + 1], device(down))
                )
            self.steps.append(copies)

    def start(self, s):
        for copy in self.steps[s]:
            copy.start()

    def arrive(self, s):
        for copy in self.steps[s]:
            copy.wait_recv()

    def relay(self, s):
        self.arrive(s)
        if s < 3:
            self.start(s + 1)

    def drain(self):
        for copies in self.steps:
            for copy in copies:
                copy.wait_send()


class Two8:
    def __init__(self, slab, i, device, send, recv):
        def to(block, step, n):
            return remote(
                block, block, send.at[n], recv.at[n], device(lax.rem(i + 8 + step, 8))
            )

        own, low, high = slab(i), slab(lax.rem(i + 6, 8)), slab(lax.rem(i + 2, 8))
        self.one = [to(own, step, n) for n, step in enumerate((1, -1, 2, -2))]
        self.two = [to(low, 1, 4), to(high, -1, 5), to(low, 2, 6)]

    def start(self):
        for copy in self.one:
            copy.start()

    def forward(self):
        for copy in self.one:
            copy.wait_recv()
        for copy in self.two:
            copy.start()

    def arrive(self):
        for copy in self.two:
            copy.wait_recv()

    def drain(self):
        for copy in self.one + self.two:
            copy.wait_send()


def layer_norm(floats, gain, shift):
    center = jnp.sum(floats, axis=-1, keepdims=True) * (1.0 / D)
    moved = floats - center
    spread = jnp.sum(moved * moved, axis=-1, keepdims=True) * (1.0 / D)
    return (moved * lax.rsqrt(spread + EPS) * gain + shift).astype(BF16)


def dot(a, b):
    return jnp.dot(a, b, preferred_element_type=F32)


def kernel(
    servers, frames_hbm, qkv_hbm, fc1_in, out_hbm, fc2_hbm, qv_hbm, bo_hbm, b1_hbm, b2_hbm,
    g1_hbm, s1_hbm, g2_hbm, s2_hbm,
    out,
    keys, slots, order, frames, qkv_in, out_in, fc2_in, b_qv, b_out, b_fc1, b_fc2, g1, s1, g2, s2,
    norms, fin, p1, pb, pm, p2, xg, wq, w1, w2, wo, tail, pair, bias, bg, xr, xn, qs, kv, cs, cx, att, n2, pk,
    ra, rb, rc, rd, fo,
    fetch, local, s_p1, r_p1, s_p2, r_p2, r_b1, r_b2, s_more, r_more, s_last, s_pair, r_pair, s_bias, r_bias,
    s_zq, r_zq, s_zo, r_zo, s_z1, r_z1, s_z2, r_z2,
    s_xq, r_xq, s_xo, r_xo, s_x1, r_x1, s_x2, r_x2,
    s_yx, r_yx, s_yo, r_yo, s_yn, r_yn, s_d, r_d, s_kv, r_kv, s_cx, r_cx, s_rs, r_rs, s_out, s_next, r_out,
):
    x, zl, c = lax.axis_index("x"), lax.axis_index("zl"), lax.axis_index("c")
    y, zh = lax.axis_index("y"), lax.axis_index("zh")
    z = zh * 4 + zl
    clip = x * 8 + zl * 2 + c

    def at(x_=x, zl_=zl, c_=c, y_=y, zh_=zh):
        return (x_, zl_, c_, y_, zh_)

    def at_z(z_):
        return at(zl_=lax.rem(z_, 4), zh_=z_ // 4)

    def at_x(i):
        return at(x_=i)

    def at_y(i):
        return at(y_=i)

    sibling = at(c_=1 - c)

    fetches = [
        pltpu.make_async_copy(src, dst, fetch.at[n])
        for n, (src, dst) in enumerate(
            [(frames_hbm, frames), (out_hbm, out_in), (fc2_hbm, fc2_in), (qkv_hbm, qkv_in),
             (qv_hbm, b_qv), (bo_hbm, b_out), (b1_hbm, b_fc1), (b2_hbm, b_fc2), (g1_hbm, g1),
             (s1_hbm, s1), (g2_hbm, g2), (s2_hbm, s2), (fc1_in, w1.at[zh, x, zl, c])]
        )
    ]
    for copy in fetches:
        copy.start()
    barrier = pltpu.get_barrier_semaphore()

    def greet(device):
        pl.semaphore_signal(barrier, inc=1, device_id=device, device_id_type=MESH)

    @pl.loop(0, 16)
    def _(i):
        t = lax.rem(x * 4 + zl + i, 16)
        greet(at(x_=t // 4, zl_=lax.rem(t, 4), zh_=1 - zh))

    @pl.loop(1, 32)
    def _(i):
        t = lax.rem(clip + i, 32)
        greet(at(x_=t // 8, zl_=lax.rem(t // 2, 4), c_=lax.rem(t, 2)))

    greet(at(c_=1 - c, zh_=1 - zh))
    for i in range(1, 4):
        greet(at(y_=lax.rem(y + i, 4)))
        greet(at(y_=lax.rem(y + i, 4), zh_=1 - zh))

    for copy in fetches:
        copy.wait()

    for half in range(2):
        for tile in range(100):
            rt, lt = half * 20 + tile // 5, tile % 5
            fin[half, tile] = frames[8 * rt : 8 * rt + 8, 128 * lt : 128 * lt + 128]
    for h in range(2):
        tail[h, 0:4] = out_in[:, 640 * h : 640 * h + 640]
        tail[h, 4:24] = fc2_in[:, 640 * h : 640 * h + 640]
    for t in range(3):
        wq[zh, x, zl, c, :, 128 * t : 128 * t + 128] = qkv_in[t]
    def flat(ref):
        return jnp.concatenate([ref[i : i + 1] for i in range(ref.shape[0])], axis=1)

    bias[0:1, :] = flat(b_fc1)
    for i, ref in enumerate((g1, s1, g2, s2)):
        norms[i : i + 1] = flat(ref)
    bias[1:2, 0:160] = b_out[...]
    bias[2:3, 0:160] = b_fc2[...]
    bias[3:5, 0:128] = b_qv[...]

    zq = Two8(lambda i: wq.at[i // 4, x, lax.rem(i, 4), c], z, at_z, s_zq, r_zq)
    zo = Two8(lambda i: wo.at[c, y, i // 4, x, lax.rem(i, 4)], z, at_z, s_zo, r_zo)
    z1 = Two8(lambda i: w1.at[i // 4, x, lax.rem(i, 4), c], z, at_z, s_z1, r_z1)
    z2 = Ring8(lambda i: w2.at[c, i // 4, :, lax.rem(i, 4)], z, at_z, s_z2, r_z2)
    xq = Ring4(lambda i: wq.at[:, i, :, c], lambda i, h: wq.at[h, i, :, c], x, at_x, s_xq, r_xq)
    xo = Ring4(lambda i: wo.at[c, y, :, i], lambda i, h: wo.at[c, y, h, i], x, at_x, s_xo, r_xo)
    x1 = Ring4(lambda i: w1.at[:, i, :, c], lambda i, h: w1.at[h, i, :, c], x, at_x, s_x1, r_x1)
    x2 = Ring4(
        lambda i: w2.at[c, zh, i, zl],
        lambda i, h: w2.at[c, zh, i, zl, pl.ds(24 * h, 24 - 8 * h)],
        x, at_x, s_x2, r_x2,
    )
    yo = Ring4(lambda i: wo.at[c, i], lambda i, h: wo.at[c, i, h], y, at_y, s_yo, r_yo)

    def yx(t):
        tiles = pl.ds(t * 20, 20)
        return Ring4(
            lambda i: xg.at[i, :, tiles], lambda i, h: xg.at[i, h, tiles], y, at_y, s_yx, r_yx, t * 4
        )

    def yn(t):
        def rows(first, count):
            return pl.ds(pl.multiple_of(t * ROWS + first, 16), count)

        return Ring4(
            lambda i: n2.at[i, rows(0, ROWS)], lambda i, h: n2.at[i, rows(16 * h, 16)],
            y, at_y, s_yn, r_yn, t * 4,
        )

    dq = remote(wq.at[:, :, :, c], wq.at[:, :, :, c], s_d.at[0], r_d.at[0], sibling)
    d1 = remote(w1.at[:, :, :, c], w1.at[:, :, :, c], s_d.at[1], r_d.at[1], sibling)
    d2 = remote(w2.at[c], w2.at[c], s_d.at[2], r_d.at[2], sibling)

    def dkv(t):
        return remote(kv.at[c, t], kv.at[c, t], s_kv.at[t], r_kv.at[t], sibling)

    do = []
    for n in range(4):
        part = wo.at[c, lax.rem(y + (0, 1, 3, 2)[n], 4)]
        do.append(remote(part, part, s_d.at[3 + n], r_d.at[3 + n], sibling))
    bias_sends = []
    for i in range(4):
        for other in range(2):
            if i or other:
                device = at(y_=lax.rem(y + i, 4), zh_=(1 - zh) if other else zh)
                n = i * 2 + other
                bias_sends.append(
                    remote(bias, bg.at[y * 2 + zh], s_bias.at[n], r_bias.at[n], device)
                )
    own_b = pltpu.make_async_copy(bias, bg.at[y * 2 + zh], local.at[1])
    own_pair = pltpu.make_async_copy(tail.at[c], pair.at[c], local.at[2])
    to_pair = remote(tail.at[1 - c], pair.at[c], s_pair, r_pair, sibling)

    pl.semaphore_wait(barrier, 54)

    to_pair.start()
    zq.start()
    own_b.start()
    own_pair.start()

    def tiles_of(x_, zl_, second):
        if second:
            return FIRST + x_ * 13 + zl_ * PART + jnp.minimum(zl_, 1)
        return (x_ * 4 + zl_) * PART

    def regroup_sends(first, last, second):
        landing, arrived_at = (p1, pb)[second], (r_p1, r_b1)[second]

        @pl.loop(first, last)
        def _(i):
            t = lax.rem(clip + i, 32)
            x_, zl_, c_ = t // 8, lax.rem(t // 2, 4), lax.rem(t, 2)
            tile = tiles_of(x_, zl_, second)
            device = at(x_=x_, zl_=zl_, c_=c_)
            remote(
                fin.at[c_, pl.ds(tile, PART)], landing.at[clip], s_p1, arrived_at, device
            ).start()
            if second:
                @pl.when(zl_ == 0)
                def _():
                    remote(
                        fin.at[c_, tile + PART], pm.at[clip], s_more, r_more, device
                    ).start()

    own_tiles = [tiles_of(x, zl, second) for second in range(2)]
    own_more = own_tiles[1] + PART
    for second in range(2):
        pltpu.make_async_copy(
            fin.at[c, pl.ds(own_tiles[second], PART)],
            (p1, pb)[second].at[clip],
            (r_p1, r_b1)[second],
        ).start()

    @pl.when(zl == 0)
    def _():
        pltpu.make_async_copy(fin.at[c, own_more], pm.at[clip], r_more).start()

    regroup_sends(1, 32, 0)
    own_pair.wait()
    to_pair.wait_recv()
    wo[c, y, zh, x, zl, 0:4] = pair[0, 0:4]
    wo[c, y, zh, x, zl, 4:8] = pair[1, 0:4]
    w2[c, zh, x, zl, 0:20] = pair[0, 4:24]
    w2[c, zh, x, zl, 20:40] = pair[1, 4:24]
    x2.start()

    for i in range(32):
        keys[i] = servers[i] * 32 + i

    @pl.loop(0, 32)
    def _(i):
        own, total = keys[i], jnp.int32(0)
        for other in range(32):
            total = total + jnp.where(keys[other] < own, 1, 0)
        slots[i] = total

    regroup_sends(1, 11, 1)
    zq.forward()
    regroup_sends(11, 32, 1)

    @pl.loop(0, 32)
    def _(i):
        total = jnp.int32(0)
        for other in range(32):
            total = total + jnp.where(slots[other] == i, other, 0)
        order[i] = total

    own_b.wait()

    slot = x * 8 + zl * 2 + zh

    def slot_sends(second):
        part, arrived_at = pl.ds(PART * second, PART), (r_p2, r_b2)[second]
        landing = (p1, pb)[second]
        pltpu.make_async_copy(landing, landing, (r_p1, r_b1)[second]).wait()

        @pl.loop(0, 32)
        def _(s):
            p2[s, part] = landing[order[s]]

        place = xg.at[y, zh, pl.ds(own_tiles[second], PART)]
        place_more = xg.at[y, zh, own_more]
        if second:
            @pl.when(zl == 0)
            def _():
                pltpu.make_async_copy(pm, pm, r_more).wait()

                @pl.loop(0, 32)
                def _(s):
                    p2[s, 2 * PART] = pm[order[s]]

        @pl.loop(1, 32)
        def _(i):
            t = lax.rem(slot + i, 32)
            device = at(x_=t // 8, zl_=lax.rem(t // 2, 4), zh_=lax.rem(t, 2))
            remote(p2.at[t, part], place, s_p2, arrived_at, device).start()
            if second:
                @pl.when(zl == 0)
                def _():
                    remote(p2.at[t, 2 * PART], place_more, s_last, arrived_at, device).start()

        pltpu.make_async_copy(p2.at[slot, part], place, arrived_at).start()
        if second:
            @pl.when(zl == 0)
            def _():
                pltpu.make_async_copy(p2.at[slot, 2 * PART], place_more, arrived_at).start()

    slot_sends(0)
    zo.start()
    zq.arrive()
    xq.start()
    slot_sends(1)
    x2.forward()
    for copy in bias_sends:
        copy.start()
    here = xg.at[y, :, pl.ds(0, FIRST)]
    pltpu.make_async_copy(here, here, r_p2).wait()
    yx(0).start()
    yx(1).start()
    zo.forward()
    z1.start()
    xq.forward()
    yx(0).forward()
    x2.arrive()
    here = xg.at[y, :, pl.ds(FIRST, TILES - FIRST)]
    pltpu.make_async_copy(here, here, r_b2).wait()
    yx(2).start()
    yx(1).forward()
    yx(3).start()
    xq.arrive()
    dq.start()
    for copy in bias_sends:
        copy.wait_recv()
    dq.wait_recv()
    zo.arrive()
    xo.start()

    def project(t):
        @pl.loop(0, 2)
        def _(u):
            first = t * 20 + u * 10
            blocks = []
            for b in range(8):
                parts = [
                    jnp.concatenate(
                        [xg[b // 2, b % 2, first + lt], xg[b // 2, b % 2, first + 5 + lt]], axis=0
                    )
                    for lt in range(5)
                ]
                blocks.append(jnp.concatenate(parts, axis=1))
            start = pl.multiple_of(t * ROWS + u * 16, 16)
            inner = pl.multiple_of(u * 16, 16)
            for j in range(4):
                whole = jnp.concatenate(
                    [block[:, 160 * j : 160 * j + 160] for block in blocks], axis=1
                )
                xr[j, pl.ds(start, 16)] = whole
                xn[j, pl.ds(inner, 16)] = layer_norm(whole.astype(F32), norms[0:1], norms[1:2])

        left = xn[...].reshape(4 * ROWS, D)
        for h in range(2):
            prod = dot(left, wq[h].reshape(D, 384))
            biases = bg[y * 2 + h]
            lanes = slice(128 * h, 128 * h + 128)
            query = ((prod[:, 0:128] + biases[3:4, 0:128]) * HDIM ** (-0.5)).astype(BF16)
            key = prod[:, 128:256].astype(BF16)
            value = (prod[:, 256:384] + biases[4:5, 0:128]).astype(BF16)
            qs[t, :, lanes] = query
            kv[c, t, 0, :, lanes] = key
            kv[c, t, 1, :, lanes] = value
        dkv(t).start()

    @pl.loop(0, CHUNKS)
    def _(t):
        with jax.named_scope("L_fwd"):
            @pl.when(t < CHUNKS - 2)
            def _():
                yx(t + 2).forward()

            @pl.when(t < CHUNKS - 4)
            def _():
                yx(t + 4).start()

        with jax.named_scope("L_z1"):
            @pl.when(t == 0)
            def _():
                z1.forward()
                z2.start(0)

            @pl.when(t == 1)
            def _():
                xo.forward()

            @pl.when(t == 2)
            def _():
                z1.arrive()
                x1.start()

            @pl.when(t == 3)
            def _():
                xo.arrive()
                yo.start()
                do[0].start()

        with jax.named_scope("L_arr"):
            yx(t).arrive()
        with jax.named_scope("L_proj"):
            project(t)

    z2.relay(0)
    for t in range(CHUNKS):
        dkv(t).wait_recv()

    head_of = lax.broadcasted_iota(jnp.int32, (4 * ROWS, 256), 1) // HDIM

    def rows_of(t):
        return pl.ds(pl.multiple_of(t * ROWS, ROWS), ROWS)

    def context_send(t, i):
        j = lax.rem(y + i, 4)
        n = 3 * t + i - 1
        return remote(cs.at[t, j], cx.at[y, rows_of(t)], s_cx.at[n], r_cx.at[n], at(y_=j))

    def attend(t):
        q = qs[t]
        zero = jnp.zeros_like(q)
        stacked = jnp.concatenate([jnp.where(head_of == h, q, zero) for h in range(4)], axis=0)
        keys = kv[:, :, 0].reshape(D, 256)
        scores = lax.dot_general(
            stacked, keys, (((1,), (1,)), ((), ())), preferred_element_type=F32
        )
        weights = jnp.exp(scores - jnp.max(scores, axis=-1, keepdims=True))
        total = jnp.sum(weights, axis=-1, keepdims=True)
        mixed = dot(weights.astype(BF16), kv[:, :, 1].reshape(D, 256)) / total
        context = jnp.zeros((4 * ROWS, 256), F32)
        for h in range(4):
            part = mixed[h * 4 * ROWS : (h + 1) * 4 * ROWS]
            context = context + jnp.where(head_of == h, part, 0.0)
        context = context.astype(BF16)
        for j in range(4):
            cs[t, j] = context[j * ROWS : (j + 1) * ROWS]
        for i in (2, 1, 3):
            context_send(t, i).start()
        cx[y, rows_of(t)] = cs[t, y]

    def whole_bias(row):
        return jnp.concatenate([bg[h, row : row + 1, 0:160] for h in range(8)], axis=1)

    def attend_out(t):
        r = rows_of(t)
        for i in range(1, 4):
            context_send(t, i).wait_recv()
        context = jnp.concatenate([cx[i, r] for i in range(4)], axis=1)
        product = jnp.concatenate(
            [dot(context, wo[h].reshape(1024, 640)) for h in range(2)], axis=1
        )
        attended = (xr[y, r].astype(F32) + whole_bias(1) + product).astype(BF16)
        att[r] = attended.astype(F32) + whole_bias(2)
        n2[y, r] = layer_norm(attended.astype(F32), norms[2:3], norms[3:4])
        yn(t).start()

    up, down, far = lax.rem(y + 1, 4), lax.rem(y + 3, 4), lax.rem(y + 2, 4)

    def sums(t):
        r, n = rows_of(t), 4 * t
        return [
            remote(pk.at[far, 0, r], ra.at[r], s_rs.at[n], r_rs.at[n], at(y_=up)),
            remote(pk.at[far, 1, r], rb.at[r], s_rs.at[n + 1], r_rs.at[n + 1], at(y_=down)),
            remote(pk.at[up, :, r], rc.at[:, r], s_rs.at[n + 2], r_rs.at[n + 2], at(y_=up)),
            remote(pk.at[down, :, r], rd.at[:, r], s_rs.at[n + 3], r_rs.at[n + 3], at(y_=down)),
        ]

    def feed_forward(t):
        r = rows_of(t)
        left = jnp.concatenate([n2[j, r] for j in range(4)], axis=0)
        parts = []
        for h in range(2):
            total = dot(left, w1[h].reshape(D, 640)) + bg[y * 2 + h, 0:1, :]
            parts.append((0.5 * total * (1.0 + lax.erf(total * 0.5**0.5))).astype(BF16))
        hidden = jnp.concatenate(parts, axis=1)

        @pl.when(t == 0)
        def _():
            d2.wait_recv()

        share = jnp.concatenate(
            [dot(hidden, w2[h].reshape(D, 640)) for h in range(2)], axis=1
        )
        kept = att[r]
        for j in range(4):
            part = share[ROWS * j : ROWS * j + ROWS] + jnp.where(y == j, kept, 0.0)
            for b in range(8):
                pk[b // 2, b % 2, r, 160 * j : 160 * j + 160] = part[
                    :, 160 * b : 160 * b + 160
                ].astype(BF16)
        sums(t)[0].start()
        sums(t)[1].start()

    def add_and_pass(t):
        r = rows_of(t)
        copies = sums(t)
        copies[0].wait_recv()
        pk[up, 0, r] = (pk[up, 0, r].astype(F32) + ra[r].astype(F32)).astype(BF16)
        copies[2].start()
        copies[1].wait_recv()
        pk[down, 1, r] = (pk[down, 1, r].astype(F32) + rb[r].astype(F32)).astype(BF16)
        copies[3].start()

    def out_rows(t):
        return out.at[pl.ds(pl.multiple_of(c * HALF + t * ROWS, ROWS), ROWS)]

    def finish(t):
        r = rows_of(t)
        copies = sums(t)
        copies[2].wait_recv()
        copies[3].wait_recv()
        fo[:, r] = (pk[y, :, r].astype(F32) + rc[:, r].astype(F32) + rd[:, r].astype(F32)).astype(
            BF16
        )
        remote(fo.at[1 - zh, r], out_rows(t), s_out, r_out, at(c_=zh, zh_=1 - zh)).start()

        @pl.when(c == zh)
        def _():
            pltpu.make_async_copy(fo.at[zh, r], out_rows(t), r_out).start()

        @pl.when(c != zh)
        def _():
            remote(fo.at[zh, r], out_rows(t), s_next, r_out, sibling).start()

    @pl.loop(0, CHUNKS)
    def _(t):
        with jax.named_scope("M_att"):
            attend(t)

        with jax.named_scope("M_w"):
            @pl.when(t == 1)
            def _():
                yo.forward()
                do[1].start()
                do[2].start()

            @pl.when(t == 2)
            def _():
                x1.forward()
                z2.relay(1)

    yo.arrive()
    do[3].start()
    for copy in do:
        copy.wait_recv()

    @pl.loop(0, CHUNKS)
    def _(t):
        with jax.named_scope("O_out"):
            attend_out(t)

        with jax.named_scope("O_z2"):
            @pl.when(t == 0)
            def _():
                z2.relay(2)
                x1.arrive()
                d1.start()

            @pl.when(t == CHUNKS - 1)
            def _():
                z2.arrive(3)
                d2.start()

        with jax.named_scope("O_fwd"):
            @pl.when(t > 1)
            def _():
                yn(t - 2).forward()

    d1.wait_recv()

    @pl.loop(0, CHUNKS + 2)
    def _(i):
        @pl.when(i < CHUNKS)
        def _():
            with jax.named_scope("M_arr"):
                yn(i).arrive()
            with jax.named_scope("M_ff"):
                feed_forward(i)
            with jax.named_scope("M_fwd"):
                @pl.when(i < 2)
                def _():
                    yn(i + 3).forward()

        with jax.named_scope("M_add"):
            @pl.when((i > 0) & (i <= CHUNKS))
            def _():
                add_and_pass(i - 1)

        with jax.named_scope("M_fin"):
            @pl.when(i > 1)
            def _():
                finish(i - 2)

    pltpu.make_async_copy(out, out, r_out).wait()

    pltpu.make_async_copy(fo.at[0], fo.at[0], s_out).wait()

    @pl.when(c != zh)
    def _():
        pltpu.make_async_copy(fo.at[0], fo.at[0], s_next).wait()

    to_pair.wait_send()
    sent = p2.at[pl.ds(0, 31), pl.ds(0, 2 * PART)]
    pltpu.make_async_copy(sent, sent, s_p1).wait()
    pltpu.make_async_copy(sent, sent, s_p2).wait()

    @pl.when(zl == 0)
    def _():
        last = p2.at[pl.ds(0, 31), 2 * PART]
        pltpu.make_async_copy(last, last, s_last).wait()
        more = pm.at[pl.ds(0, 7)]
        pltpu.make_async_copy(more, more, s_more).wait()

    @pl.when(zl != 0)
    def _():
        more = pm.at[pl.ds(0, 8)]
        pltpu.make_async_copy(more, more, s_more).wait()

    for copy in bias_sends + do + [dq, d1, d2]:
        copy.wait_send()
    for ring in (zq, zo, z1, z2, xq, xo, x1, x2, yo):
        ring.drain()

    @pl.loop(0, CHUNKS)
    def _(t):
        yx(t).drain()
        dkv(t).wait_send()
        yn(t).drain()
        for i in range(1, 4):
            context_send(t, i).wait_send()
        for copy in sums(t):
            copy.wait_send()


def on_device(
    frames_in, ln1_gain, ln1_bias, qkv_weight, qv_bias, out_weight, out_bias,
    ln2_gain, ln2_bias, fc1_weight, fc1_bias, fc2_weight, fc2_bias, server_of_clip,
):
    smem = pl.BlockSpec(memory_space=pltpu.SMEM)
    dma = pltpu.SemaphoreType.DMA
    V = pltpu.VMEM
    out = pl.pallas_call(
        kernel,
        out_shape=jax.ShapeDtypeStruct((320, 640), BF16),
        in_specs=[smem] + [pl.BlockSpec(memory_space=pl.ANY)] * 13,
        out_specs=pl.BlockSpec(memory_space=pl.ANY),
        scratch_shapes=[
            pltpu.SMEM((32,), jnp.int32), pltpu.SMEM((32,), jnp.int32), pltpu.SMEM((32,), jnp.int32),
            V((320, 640), BF16), V((3, 40, 128), BF16), V((4, D), BF16), V((20, D), BF16),
            V((2, 128), F32), V((1, 160), F32), V((5, 128), F32), V((1, 160), F32),
            V((10, 128), F32), V((10, 128), F32), V((10, 128), F32), V((10, 128), F32),
            V((4, D), F32),
            V((2, TILES, 8, 128), BF16),
            V((32, PART, 8, 128), BF16),
            V((32, PART, 8, 128), BF16),
            V((32, 8, 128), BF16),
            V((32, 2 * PART + 1, 8, 128), BF16),
            V((4, 2, TILES, 8, 128), BF16),
            V((2, 4, 4, 2, 40, 384), BF16),
            V((2, 4, 4, 2, 40, 640), BF16),
            V((2, 2, 4, 4, 40, 640), BF16),
            V((2, 4, 2, 4, 4, 8, 640), BF16),
            V((2, 24, 640), BF16),
            V((2, 24, 640), BF16),
            V((8, 640), F32),
            V((8, 8, 640), F32),
            V((4, HALF, D), BF16),
            V((4, ROWS, D), BF16),
            V((CHUNKS, 4 * ROWS, 256), BF16),
            V((2, CHUNKS, 2, 4 * ROWS, 256), BF16),
            V((CHUNKS, 4, ROWS, 256), BF16),
            V((4, HALF, 256), BF16),
            V((HALF, D), F32),
            V((4, HALF, D), BF16),
            V((4, 2, HALF, 640), BF16),
            V((HALF, 640), BF16),
            V((HALF, 640), BF16),
            V((2, HALF, 640), BF16),
            V((2, HALF, 640), BF16),
            V((2, HALF, 640), BF16),
            dma((13,)), dma((3,)),
            dma, dma, dma, dma, dma, dma, dma, dma, dma, dma, dma, dma((8,)), dma((8,)),
            dma((7,)), dma((7,)), dma((7,)), dma((7,)), dma((7,)), dma((7,)), dma((7,)), dma((7,)),
            dma((4,)), dma((4,)), dma((4,)), dma((4,)), dma((4,)), dma((4,)), dma((4,)), dma((4,)),
            dma((4 * CHUNKS,)), dma((4 * CHUNKS,)), dma((4,)), dma((4,)),
            dma((4 * CHUNKS,)), dma((4 * CHUNKS,)),
            dma((8,)), dma((8,)), dma((CHUNKS,)), dma((CHUNKS,)), dma((3 * CHUNKS,)), dma((3 * CHUNKS,)), dma((4 * CHUNKS,)), dma((4 * CHUNKS,)),
            dma, dma, dma,
        ],
        compiler_params=pltpu.CompilerParams(
            collective_id=0, has_side_effects=True, vmem_limit_bytes=60 * 2**20
        ),
    )(
        server_of_clip, frames_in.reshape(320, 640), qkv_weight.transpose(1, 0, 2), fc1_weight,
        out_weight, fc2_weight, qv_bias, out_bias[None], fc1_bias.reshape(5, 128), fc2_bias[None],
        ln1_gain.reshape(10, 128), ln1_bias.reshape(10, 128),
        ln2_gain.reshape(10, 128), ln2_bias.reshape(10, 128),
    )
    return out.reshape(1, 1, 320, 640)


def solution(mesh):
    torus = Mesh(mesh.devices.reshape(4, 4, 2, 4, 2), ("x", "zl", "c", "y", "zh"))
    return jax.shard_map(
        on_device,
        mesh=torus,
        in_specs=(
            P(DP, HEAD, None, None), P(), P(), P(DP, None, HEAD), P(None, HEAD), P(HEAD_DP, None),
            P(HEAD), P(), P(), P(DP, HEAD), P(HEAD), P(HEAD_DP, None), P(HEAD), P(),
        ),
        out_specs=P(DP, HEAD, None, None),
        check_vma=False,
    )
```
